512 devices in a mesh: pts: 32 (over x, y, core), cand: 16 (over z).
Axes of the slice: x: 4, y: 4, z: 16, core: 2. Of those that a mesh axis runs over, the one named last changes fastest.
Arguments:
- points: bfloat16 [32768, 1024], P('pts'), may hold values from -6 to 6
- weights: float32 [32768], P('pts'), may hold values from 0.5 to 5
- coverage: float32 [32768], P('pts'), may hold values from -0.5 to 1
- candidates: bfloat16 [16384, 1024], P('cand'), may hold values from -6 to 6
- picks: int32 [64], replicated, may hold values from 0 to 16383
Outputs:
- gains: float32 [16384], P('cand')
- top_gains: float32 [64], replicated
- new_coverage: float32 [32768], P('pts')
The draws below stay inside these ranges and needn't reach their ends.
All inputs are finite; a program needn't handle non-finite values.
Results may differ from the reference program's by a relative error of at most 0.0003.
Values may be sent and summed in bfloat16 or wider, within the bound.
A program may use at most 64 MiB of HBM per device.

```python
import math
import jax
import jax.numpy as jnp
from jax import lax

D = 1024
CAND_DEV = 1024
NPICK = 64
TOPK = 64
NPTS = 32768
NCAND = 16384
N_CAND = 16


def set_ends(result, rng, smallest, top_value):
    dims = result.shape
    place = [jax.random.randint(jax.random.fold_in(rng, axis), (), 0, dims[axis]) for axis in range(len(dims))]
    result = result.at[tuple(place)].set(smallest)
    longest = dims.index(max(dims))
    place[longest] = (place[longest] + 1) % dims[longest]
    return result.at[tuple(place)].set(top_value)


def block_levels(stream_key, dims, shards, smallest, largest):
    def one(position, parts):
        heights = jax.random.uniform(jax.random.fold_in(jax.random.fold_in(stream_key, 6), position), (parts,), jnp.float32, smallest / len(shards), largest / len(shards))
        return jnp.repeat(jnp.exp(heights), dims[position] // parts).reshape((-1,) + (1,) * (len(dims) - position - 1))

    gain = one(*shards[0])
    for cut in shards[1:]:
        gain = gain * one(*cut)
    return gain


def noise(key, shape, width, most, shards=(), dtype=jnp.bfloat16):
    entries = jax.random.normal(key, shape, jnp.float32) * width
    if len(shards) > 0:
        entries = block_levels(key, shape, shards, -0.22, 0.18) * entries
    return jnp.clip(entries, min=-most, max=most).astype(dtype)


def setup_inputs(seed: int = 0) -> dict:
    key_of = jax.random.split(jax.random.key(seed), 6)
    return {
        "points": noise(key_of[0], (NPTS, D), 1.0, 6.0, ((0, 32),)),
        "weights": jnp.clip(jnp.exp(math.log(5.0) - 2.3025851 * jax.random.uniform(key_of[1], (NPTS,), jnp.float32) ** block_levels(key_of[1], (NPTS,), ((0, 32),), -0.2, 0.2)), 0.5, 5.0),
        "coverage": jnp.clip(-0.5 + 1.5 * jax.random.uniform(key_of[2], (NPTS,), jnp.float32) ** block_levels(key_of[2], (NPTS,), ((0, 32),), -0.2, 0.2), -0.5, 1.0),
        "candidates": noise(key_of[3], (NCAND, D), 1.0, 6.0, ((0, 16),)),
        "picks": set_ends(jax.random.randint(key_of[4], (NPICK,), 0, NCAND), jax.random.fold_in(key_of[4], 1), 0, NCAND - 1).astype(jnp.int32),
    }


def reference(points, weights, coverage, candidates, picks):
    scale = D ** -0.5
    total = points.shape[0]
    blocks = candidates.reshape(N_CAND, CAND_DEV, D)

    def block_gain(block):
        sims = jnp.dot(points, block.T, preferred_element_type=jnp.float32) * scale
        return jnp.sum(weights[:, None] * jnp.maximum(sims - coverage[:, None], 0.0), axis=0) / total

    gains = lax.map(block_gain, blocks).reshape(-1)
    top_gains = lax.top_k(gains, TOPK)[0]
    picked = jnp.take(candidates, picks.astype(jnp.int32), axis=0)
    picked_sims = jnp.dot(points, picked.T, preferred_element_type=jnp.float32) * scale
    new_coverage = jnp.maximum(coverage, jnp.max(picked_sims, axis=1))
    return gains, top_gains, new_coverage
```

```python
import functools

import jax
import jax.numpy as jnp
from jax import lax
from jax.experimental import pallas as pl
from jax.experimental.pallas import tpu as pltpu
from jax.sharding import PartitionSpec as P

TOPK = 64
LANES = 128
F32 = jnp.float32


def column_of(row):
    return jnp.broadcast_to(row, (LANES, LANES)).T


def best_sorted(rows_ref, col_ref):
    for k in range(8):
        col_ref[k * LANES:(k + 1) * LANES, :] = column_of(rows_ref[k:k + 1, :])
    rows = [jnp.broadcast_to(rows_ref[k:k + 1, :], (8, LANES)) for k in range(8)]

    def count(step, above):
        for part in range(8):
            start = pl.multiple_of(step * 64 + part * 8, 8)
            other = col_ref[pl.ds(start, 8), :]
            above = tuple(a + jnp.where(other > r, 1.0, 0.0) for a, r in zip(above, rows))
        return above

    above = lax.fori_loop(0, 16, count, tuple(jnp.zeros((8, LANES), F32) for _ in range(8)))
    above = [jnp.broadcast_to(jnp.sum(a, axis=0, keepdims=True), (8, LANES)) for a in above]
    sub = lax.broadcasted_iota(jnp.int32, (8, LANES), 0)
    lane = lax.rem(lax.broadcasted_iota(jnp.int32, (8, LANES), 1), TOPK)
    placed = jnp.zeros((8, LANES), F32)
    for block in range(8):
        place = (sub + block * 8).astype(F32)
        best = jnp.full((8, LANES), jnp.inf, F32)
        for a, r in zip(above, rows):
            best = jnp.minimum(best, jnp.where(a <= place, r, jnp.inf))
        best = jnp.min(best, axis=1, keepdims=True)
        placed = placed + jnp.where(lane == sub + block * 8, best, 0.0)
    return jnp.sum(placed, axis=0, keepdims=True)


def kernel(
    n_pts, n_cand,
    points_hbm, weights_hbm, cover_hbm, cand_hbm, picks_hbm,
    gains_ref, top_ref, ncov_ref,
    points, cands, weights, cover, picks, wcol, ccol, bias, maxes, acc, col,
    part_out, part_in, cov_out, cov_in, top_out, top_in, rows,
    in_sem, p_send, p_recv, c_send, c_recv, t_send, t_recv,
):
    n = points.shape[0]
    m = cands.shape[0]
    me_p = lax.axis_index("pts")
    me_c = lax.axis_index("cand")

    copies = [
        pltpu.make_async_copy(cover_hbm, cover, in_sem.at[0]),
        pltpu.make_async_copy(weights_hbm, weights, in_sem.at[1]),
        pltpu.make_async_copy(picks_hbm, picks, in_sem.at[2]),
        pltpu.make_async_copy(cand_hbm.at[pl.ds(0, 256)], cands.at[pl.ds(0, 256)], in_sem.at[3]),
        pltpu.make_async_copy(points_hbm, points, in_sem.at[4]),
        pltpu.make_async_copy(cand_hbm.at[pl.ds(256, 768)], cands.at[pl.ds(256, 768)], in_sem.at[5]),
    ]
    for copy in copies:
        copy.start()

    barrier = pltpu.get_barrier_semaphore()
    for k in range(1, n_pts):
        pl.semaphore_signal(barrier, 1, device_id={"pts": lax.rem(me_p + k, n_pts)}, device_id_type=pl.DeviceIdType.MESH)
    for k in range(1, n_cand):
        pl.semaphore_signal(barrier, 1, device_id={"cand": lax.rem(me_c + k, n_cand)}, device_id_type=pl.DeviceIdType.MESH)

    copies[0].wait()
    copies[1].wait()
    for k in range(8):
        ccol[k * LANES:(k + 1) * LANES, :] = column_of(cover[k:k + 1, :] * 32.0)
        wcol[k * LANES:(k + 1) * LANES, :] = column_of(weights[k:k + 1, :] * (2.0 ** -20))
    copies[2].wait()
    column = (
        me_c * m
        + lax.broadcasted_iota(jnp.int32, (8, LANES), 0) * LANES
        + lax.broadcasted_iota(jnp.int32, (8, LANES), 1)
    )
    mask = jnp.full((8, LANES), -1e30, F32)
    for k in range(TOPK):
        mask = jnp.where(column == picks[k], 0.0, mask)
    bias[...] = mask
    copies[3].wait()
    copies[4].wait()

    block = 256
    for tile in range(4):
        if tile == 1:
            copies[5].wait()
        rhs = cands[tile * 256:(tile + 1) * 256, :]
        halves = [bias[2 * tile + h:2 * tile + h + 1, :] for h in range(2)]
        sums = [jnp.zeros((8, LANES), F32) for _ in range(2)]
        for b in range(n // block):
            at = slice(b * block, (b + 1) * block)
            sims = lax.dot_general(
                points[at, :], rhs, (((1,), (1,)), ((), ())), preferred_element_type=F32
            )
            high = None
            for h in range(2):
                s = sims[:, h * LANES:(h + 1) * LANES]
                t = jnp.maximum(s - ccol[at, :], 0.0) * wcol[at, :]
                sums[h] = sums[h] + jnp.sum(t.reshape(block // 8, 8, LANES), axis=0)
                masked = s + halves[h]
                high = masked if high is None else jnp.maximum(high, masked)
            if tile == 0:
                maxes[at, :] = high
            else:
                maxes[at, :] = jnp.maximum(maxes[at, :], high)
        for h in range(2):
            part_out[2 * tile + h:2 * tile + h + 1, :] = jnp.sum(sums[h], axis=0, keepdims=True)

    pl.semaphore_wait(barrier, n_pts - 1 + n_cand - 1)
    part_in[me_p] = part_out[...]
    for k in range(1, n_pts):
        pltpu.make_async_remote_copy(
            part_out, part_in.at[me_p], p_send, p_recv,
            device_id={"pts": lax.rem(me_p + k, n_pts)}, device_id_type=pl.DeviceIdType.MESH,
        ).start()
    for k in range(8):
        high = maxes[k * LANES:(k + 1) * LANES, :].T
        cov_out[k:k + 1, :] = jnp.max(high, axis=0, keepdims=True) * (2.0 ** -5)
    cov_in[me_c] = cov_out[...]
    for k in range(1, n_cand):
        pltpu.make_async_remote_copy(
            cov_out, cov_in.at[me_c], c_send, c_recv,
            device_id={"cand": lax.rem(me_c + k, n_cand)}, device_id_type=pl.DeviceIdType.MESH,
        ).start()

    some = part_in.at[pl.ds(0, n_pts - 1)]
    pltpu.make_async_copy(some, some, p_recv).wait()
    total = part_in[0]
    for k in range(1, n_pts):
        total = total + part_in[k]
    rows[...] = total
    gains_ref[...] = total
    top_out[...] = best_sorted(rows, col)
    top_in[me_c] = top_out[...]
    for k in range(1, n_cand):
        pltpu.make_async_remote_copy(
            top_out, top_in.at[me_c], t_send, t_recv,
            device_id={"cand": lax.rem(me_c + k, n_cand)}, device_id_type=pl.DeviceIdType.MESH,
        ).start()

    some = cov_in.at[pl.ds(0, n_cand - 1)]
    pltpu.make_async_copy(some, some, c_recv).wait()
    best = cover[...]
    for k in range(n_cand):
        best = jnp.maximum(best, cov_in[k])
    ncov_ref[...] = best

    some = top_in.at[pl.ds(0, n_cand - 1)]
    pltpu.make_async_copy(some, some, t_recv).wait()
    left = lax.broadcasted_iota(jnp.int32, (1, LANES), 1) < TOPK
    for k in range(8):
        rows[k:k + 1, :] = jnp.where(left, top_in[2 * k], top_in[2 * k + 1])
    top_ref[...] = best_sorted(rows, col)[:, :TOPK]

    some = part_in.at[pl.ds(0, n_pts - 1)]
    pltpu.make_async_copy(some, some, p_send).wait()
    some = cov_in.at[pl.ds(0, n_cand - 1)]
    pltpu.make_async_copy(some, some, c_send).wait()
    some = top_in.at[pl.ds(0, n_cand - 1)]
    pltpu.make_async_copy(some, some, t_send).wait()


def on_device(points, weights, coverage, candidates, picks):
    n_pts, n_cand = lax.axis_size("pts"), lax.axis_size("cand")
    n, d = points.shape
    m = candidates.shape[0]
    hbm = pl.BlockSpec(memory_space=pl.ANY)
    vmem = pl.BlockSpec(memory_space=pltpu.VMEM)
    dma = pltpu.SemaphoreType.DMA
    gains, top, ncov = pl.pallas_call(
        functools.partial(kernel, n_pts, n_cand),
        out_shape=(
            jax.ShapeDtypeStruct((8, LANES), F32),
            jax.ShapeDtypeStruct((1, TOPK), F32),
            jax.ShapeDtypeStruct((8, LANES), F32),
        ),
        in_specs=[hbm] * 5,
        out_specs=(vmem, vmem, vmem),
        scratch_shapes=[
            pltpu.VMEM((n, d), jnp.bfloat16),
            pltpu.VMEM((m, d), jnp.bfloat16),
            pltpu.VMEM((8, LANES), F32),
            pltpu.VMEM((8, LANES), F32),
            pltpu.SMEM((TOPK,), jnp.int32),
            pltpu.VMEM((n, LANES), F32),
            pltpu.VMEM((n, LANES), F32),
            pltpu.VMEM((8, LANES), F32),
            pltpu.VMEM((n, LANES), F32),
            pltpu.VMEM((8, 256), F32),
            pltpu.VMEM((1024, LANES), F32),
            pltpu.VMEM((8, LANES), F32),
            pltpu.VMEM((n_pts, 8, LANES), F32),
            pltpu.VMEM((8, LANES), F32),
            pltpu.VMEM((n_cand, 8, LANES), F32),
            pltpu.VMEM((1, LANES), F32),
            pltpu.VMEM((n_cand, 1, LANES), F32),
            pltpu.VMEM((8, LANES), F32),
            dma((6,)), dma, dma, dma, dma, dma, dma,
        ],
        compiler_params=pltpu.CompilerParams(collective_id=0, has_side_effects=True, vmem_limit_bytes=60 * 2**20),
        name="facility",
    )(points, weights.reshape(8, LANES), coverage.reshape(8, LANES), candidates, picks)
    return gains.reshape(m), top.reshape(TOPK), ncov.reshape(n)


def solution(mesh):
    placed = (P("pts", None), P("pts"), P("pts"), P("cand", None), P())
    return jax.shard_map(
        on_device, mesh=mesh, in_specs=placed, out_specs=(P("cand"), P(), P("pts")), check_vma=False
    )
```

```python
import functools

import jax
import jax.numpy as jnp
from jax import lax
from jax.experimental import pallas as pl
from jax.experimental.pallas import tpu as pltpu
from jax.sharding import PartitionSpec as P

TOPK = 64
LANES = 128
F32 = jnp.float32
VMEM_BYTES = 56557568 - 70 * 1024


def column_of(row):
    return jnp.broadcast_to(row, (LANES, LANES)).T


def descending(rows):
    rows, n, p = list(rows), len(rows), 1
    while p < n:
        k = p
        while k >= 1:
            for j in range(k % p, n - k, 2 * k):
                for i in range(min(k, n - j - k)):
                    if (i + j) // (2 * p) == (i + j + k) // (2 * p):
                        x, y = rows[i + j], rows[i + j + k]
                        rows[i + j], rows[i + j + k] = jnp.maximum(x, y), jnp.minimum(x, y)
            k //= 2
        p *= 2
    return rows


def wide(row):
    return jnp.broadcast_to(row, (8, LANES))


def number_above(columns, row):
    total = jnp.zeros((8, LANES), F32)
    for column in columns:
        total = total + jnp.where(column > row, 1.0, 0.0)
    return wide(jnp.sum(total, axis=0, keepdims=True))


def placed(pairs, blocks, sub):
    result = []
    for block in range(blocks):
        place = sub + float(block * 8)
        best = jnp.full((8, LANES), jnp.inf, F32)
        for row, above in pairs:
            best = jnp.minimum(best, jnp.where(above <= place, row, jnp.inf))
        result.append(jnp.broadcast_to(jnp.min(best, axis=1, keepdims=True), (8, LANES)))
    return result


def as_row(blocks, sub, lane):
    total = jnp.zeros((8, LANES), F32)
    for index, block in enumerate(blocks):
        total = total + jnp.where(lane == sub + float(index * 8), block, 0.0)
    return jnp.sum(total, axis=0, keepdims=True)


def positions():
    sub = lax.broadcasted_iota(jnp.int32, (8, LANES), 0).astype(F32)
    lane = lax.broadcasted_iota(jnp.int32, (8, LANES), 1)
    return sub, lane.astype(F32), lax.rem(lane, TOPK).astype(F32)


def order_pair(rows, columns):
    sub, _, twice = positions()
    pairs = [(wide(row), number_above(columns, wide(row))) for row in rows]
    return as_row(placed(pairs, TOPK // 8, sub), sub, twice)


def best_of_block(total_ref, col_ref):
    sub, lane, _ = positions()
    rows = descending([total_ref[k:k + 1, :] for k in range(8)])
    for k, row in enumerate(rows):
        col_ref[k * LANES:(k + 1) * LANES, :] = column_of(row)
    kept = []
    for k, row in enumerate(rows):
        columns = [col_ref[k * LANES + 8 * j:k * LANES + 8 * j + 8, :] for j in range(16)]
        above = number_above(columns, wide(row))
        kept += placed([(wide(row), above)], -(-(TOPK // (k + 1)) // 8), sub)
    first = as_row(kept[:16], sub, lane)
    second = jnp.where(lane[:1] < 8.0 * (len(kept) - 16), as_row(kept[16:], sub, lane), -jnp.inf)
    return order_pair([first, second], kept)


def best_of_lists(lists, col_ref):
    lane = lax.broadcasted_iota(jnp.int32, (1, LANES), 1)
    rows = descending(lists)
    low = jnp.full((1, LANES), -jnp.inf, F32)
    packed = []
    for group in ((0, 1, 2, 5), (3, 4) + tuple(range(6, len(rows)))):
        at, line = 0, low
        for s in group:
            count = TOPK // (s + 1)
            moved = rows[s] if at % TOPK == 0 else pltpu.roll(rows[s], at, 1)
            line = jnp.where((lane >= at) & (lane < at + count), moved, line)
            at += count
        packed.append((line, at))
    columns = []
    for k, (line, used) in enumerate(packed):
        col_ref[k * LANES:(k + 1) * LANES, :] = column_of(line)
        columns += [col_ref[k * LANES + 8 * j:k * LANES + 8 * j + 8, :] for j in range(-(-used // 8))]
    return order_pair([line for line, _ in packed], columns)


def kernel(n_pts, n_cand, points_hbm, weights_hbm, cover_hbm, cand_hbm, picks_hbm, *refs):
    gains_refs, ncov_refs, top_ref = refs[:8], refs[8:16], refs[16]
    (
        points, cands, weights, cover, picks, wcol, ccol, bias, maxes, col,
        part_out, part_in, cov_out, cov_in, top_out, top_in, gains,
        in_sem, p_send, p_recv, c_send, c_recv, t_send, t_recv, near_sem,
    ) = refs[17:]
    n = points.shape[0]
    m = cands.shape[0]
    me_p = lax.axis_index("pts")
    me_c = lax.axis_index("cand")

    copies = [
        pltpu.make_async_copy(cover_hbm, cover, in_sem.at[0]),
        pltpu.make_async_copy(weights_hbm, weights, in_sem.at[1]),
        pltpu.make_async_copy(picks_hbm, picks, in_sem.at[2]),
        pltpu.make_async_copy(cand_hbm.at[pl.ds(0, 256)], cands.at[pl.ds(0, 256)], in_sem.at[3]),
        pltpu.make_async_copy(points_hbm, points, in_sem.at[4]),
        pltpu.make_async_copy(cand_hbm.at[pl.ds(256, 768)], cands.at[pl.ds(256, 768)], in_sem.at[5]),
    ]
    for copy in copies:
        copy.start()

    barrier = pltpu.get_barrier_semaphore()
    for k in range(1, n_pts):
        pl.semaphore_signal(barrier, 1, device_id={"pts": lax.rem(me_p + k, n_pts)}, device_id_type=pl.DeviceIdType.MESH)
    for k in (1, n_cand - 1):
        pl.semaphore_signal(barrier, 1, device_id={"cand": lax.rem(me_c + k, n_cand)}, device_id_type=pl.DeviceIdType.MESH)

    copies[0].wait()
    copies[1].wait()
    for k in range(8):
        ccol[k * LANES:(k + 1) * LANES, :] = column_of(cover[k:k + 1, :] * 32.0)
        wcol[k * LANES:(k + 1) * LANES, :] = column_of(weights[k:k + 1, :] * (2.0 ** -20))
    copies[2].wait()
    column = (
        me_c * m
        + lax.broadcasted_iota(jnp.int32, (8, LANES), 0) * LANES
        + lax.broadcasted_iota(jnp.int32, (8, LANES), 1)
    )
    mask = jnp.full((8, LANES), -1e30, F32)
    for k in range(TOPK):
        mask = jnp.where(column == picks[k], 0.0, mask)
    bias[...] = mask
    copies[3].wait()
    copies[4].wait()

    block = 256
    for tile in range(4):
        if tile == 1:
            copies[5].wait()
        rhs = cands[tile * 256:(tile + 1) * 256, :]
        halves = [bias[2 * tile + h:2 * tile + h + 1, :] for h in range(2)]
        sums = [jnp.zeros((8, LANES), F32) for _ in range(2)]
        for b in range(n // block):
            at = slice(b * block, (b + 1) * block)
            sims = lax.dot_general(
                points[at, :], rhs, (((1,), (1,)), ((), ())), preferred_element_type=F32
            )
            high = None
            for h in range(2):
                s = sims[:, h * LANES:(h + 1) * LANES]
                t = jnp.maximum(s - ccol[at, :], 0.0) * wcol[at, :]
                sums[h] = sums[h] + jnp.sum(t.reshape(block // 8, 8, LANES), axis=0)
                masked = s + halves[h]
                high = masked if high is None else jnp.maximum(high, masked)
            if tile == 0:
                maxes[at, :] = high
            else:
                maxes[at, :] = jnp.maximum(maxes[at, :], high)
        for h in range(2):
            part_out[2 * tile + h:2 * tile + h + 1, :] = jnp.sum(sums[h], axis=0, keepdims=True)

    pl.semaphore_wait(barrier, n_pts + 1)
    part_in[me_p] = part_out[...]
    for k in range(1, n_pts):
        pltpu.make_async_remote_copy(
            part_out, part_in.at[me_p], p_send, p_recv,
            device_id={"pts": lax.rem(me_p + k, n_pts)}, device_id_type=pl.DeviceIdType.MESH,
        ).start()
    reach, rounds = 1, 0
    while reach < n_cand // 2:
        for k in (reach, n_cand - reach):
            pl.semaphore_signal(
                near_sem.at[rounds], 1, device_id={"cand": lax.rem(me_c + k, n_cand)}, device_id_type=pl.DeviceIdType.MESH
            )
        if rounds == 0:
            for k in range(8):
                high = maxes[k * LANES:(k + 1) * LANES, :].T
                cov_out[k:k + 1, :] = jnp.max(high, axis=0, keepdims=True) * (2.0 ** -5)
        pl.semaphore_wait(near_sem.at[rounds], 2)
        reach, rounds = 2 * reach, rounds + 1
    for k in range(1, n_cand):
        pltpu.make_async_remote_copy(
            cov_out, cov_in.at[k], c_send, c_recv,
            device_id={"cand": lax.rem(me_c + k, n_cand)}, device_id_type=pl.DeviceIdType.MESH,
        ).start()

    some = part_in.at[pl.ds(0, n_pts - 1)]
    pltpu.make_async_copy(some, some, p_recv).wait()
    total = part_in[0]
    for k in range(1, n_pts):
        total = total + part_in[k]
    gains[...] = total
    top_out[...] = best_of_block(gains, col)
    for k in range(1, n_cand):
        pltpu.make_async_remote_copy(
            top_out, top_in.at[k], t_send, t_recv,
            device_id={"cand": lax.rem(me_c + k, n_cand)}, device_id_type=pl.DeviceIdType.MESH,
        ).start()

    some = cov_in.at[pl.ds(1, n_cand - 1)]
    pltpu.make_async_copy(some, some, c_recv).wait()
    best = jnp.maximum(cover[...], cov_out[...])
    for k in range(1, n_cand):
        best = jnp.maximum(best, cov_in[k])
    for k in range(8):
        gains_refs[k][...] = gains[k:k + 1, :]
        ncov_refs[k][...] = best[k:k + 1, :]

    for sent, sem, count in ((part_in, p_send, n_pts - 1), (cov_in, c_send, n_cand - 1), (top_in, t_send, n_cand - 1)):
        some = sent.at[pl.ds(0, count)]
        pltpu.make_async_copy(some, some, sem).wait()

    some = top_in.at[pl.ds(1, n_cand - 1)]
    pltpu.make_async_copy(some, some, t_recv).wait()
    best = best_of_lists([top_out[...]] + [top_in[k] for k in range(1, n_cand)], col)
    top_ref[...] = best


def write_out(*refs):
    rows, (gains, ncov, top), (best, sem) = refs[:17], refs[17:20], refs[20:]
    best[...] = rows[16][:, :TOPK]
    copies = [pltpu.make_async_copy(best, top, sem.at[16])]
    for k in range(8):
        copies.append(pltpu.make_async_copy(rows[k], gains.at[pl.ds(k, 1)], sem.at[k]))
        copies.append(pltpu.make_async_copy(rows[8 + k], ncov.at[pl.ds(k, 1)], sem.at[8 + k]))
    for copy in copies:
        copy.start()
    for copy in copies:
        copy.wait()


def on_device(points, weights, coverage, candidates, picks):
    n_pts, n_cand = lax.axis_size("pts"), lax.axis_size("cand")
    n, d = points.shape
    m = candidates.shape[0]
    hbm = pl.BlockSpec(memory_space=pl.ANY)
    vmem = pl.BlockSpec(memory_space=pltpu.VMEM)
    dma = pltpu.SemaphoreType.DMA
    inside = pl.pallas_call(
        functools.partial(kernel, n_pts, n_cand),
        out_shape=(jax.ShapeDtypeStruct((1, LANES), F32),) * 17,
        in_specs=[hbm] * 5,
        out_specs=(vmem,) * 17,
        scratch_shapes=[
            pltpu.VMEM((n, d), jnp.bfloat16),
            pltpu.VMEM((m, d), jnp.bfloat16),
            pltpu.VMEM((8, LANES), F32),
            pltpu.VMEM((8, LANES), F32),
            pltpu.SMEM((TOPK,), jnp.int32),
            pltpu.VMEM((n, LANES), F32),
            pltpu.VMEM((n, LANES), F32),
            pltpu.VMEM((8, LANES), F32),
            pltpu.VMEM((n, LANES), F32),
            pltpu.VMEM((1024, LANES), F32),
            pltpu.VMEM((8, LANES), F32),
            pltpu.VMEM((n_pts, 8, LANES), F32),
            pltpu.VMEM((8, LANES), F32),
            pltpu.VMEM((n_cand, 8, LANES), F32),
            pltpu.VMEM((1, LANES), F32),
            pltpu.VMEM((n_cand, 1, LANES), F32),
            pltpu.VMEM((8, LANES), F32),
            dma((6,)), dma, dma, dma, dma, dma, dma, pltpu.SemaphoreType.REGULAR((3,)),
        ],
        compiler_params=pltpu.CompilerParams(
            collective_id=0, has_side_effects=True, vmem_limit_bytes=VMEM_BYTES
        ),
        name="facility",
    )(points, weights.reshape(8, LANES), coverage.reshape(8, LANES), candidates, picks)
    gains, ncov, top = pl.pallas_call(
        write_out,
        out_shape=(
            jax.ShapeDtypeStruct((8, LANES), F32),
            jax.ShapeDtypeStruct((8, LANES), F32),
            jax.ShapeDtypeStruct((1, TOPK), F32),
        ),
        in_specs=[vmem] * 17,
        out_specs=(hbm, hbm, hbm),
        scratch_shapes=[pltpu.VMEM((1, TOPK), F32), dma((17,))],
        compiler_params=pltpu.CompilerParams(vmem_limit_bytes=2**20),
        name="write_out",
    )(*inside)
    return gains.reshape(m), top.reshape(TOPK), ncov.reshape(n)


def solution(mesh):
    placed = (P("pts", None), P("pts"), P("pts"), P("cand", None), P())
    return jax.shard_map(
        on_device, mesh=mesh, in_specs=placed, out_specs=(P("cand"), P(), P("pts")), check_vma=False
    )
```

```python
import functools

import jax
import jax.numpy as jnp
from jax import lax
from jax.experimental import pallas as pl
from jax.experimental.pallas import tpu as pltpu
from jax.sharding import PartitionSpec as P

TOPK = 64
LANES = 128
F32 = jnp.float32
VMEM_BYTES = 56557568 - 70 * 1024


def column_of(row):
    return jnp.broadcast_to(row, (LANES, LANES)).T


def descending(rows):
    rows, n, p = list(rows), len(rows), 1
    while p < n:
        k = p
        while k >= 1:
            for j in range(k % p, n - k, 2 * k):
                for i in range(min(k, n - j - k)):
                    if (i + j) // (2 * p) == (i + j + k) // (2 * p):
                        x, y = rows[i + j], rows[i + j + k]
                        rows[i + j], rows[i + j + k] = jnp.maximum(x, y), jnp.minimum(x, y)
            k //= 2
        p *= 2
    return rows


def wide(row):
    return jnp.broadcast_to(row, (8, LANES))


def number_above(columns, row):
    total = jnp.zeros((8, LANES), F32)
    for column in columns:
        total = total + jnp.where(column > row, 1.0, 0.0)
    return wide(jnp.sum(total, axis=0, keepdims=True))


def placed(pairs, blocks, sub):
    result = []
    for block in range(blocks):
        place = sub + float(block * 8)
        best = jnp.full((8, LANES), jnp.inf, F32)
        for row, above in pairs:
            best = jnp.minimum(best, jnp.where(above <= place, row, jnp.inf))
        result.append(jnp.broadcast_to(jnp.min(best, axis=1, keepdims=True), (8, LANES)))
    return result


def as_row(blocks, sub, lane):
    total = jnp.zeros((8, LANES), F32)
    for index, block in enumerate(blocks):
        total = total + jnp.where(lane == sub + float(index * 8), block, 0.0)
    return jnp.sum(total, axis=0, keepdims=True)


def positions():
    sub = lax.broadcasted_iota(jnp.int32, (8, LANES), 0).astype(F32)
    lane = lax.broadcasted_iota(jnp.int32, (8, LANES), 1)
    return sub, lane.astype(F32), lax.rem(lane, TOPK).astype(F32)


def order_pair(rows, columns):
    sub, _, twice = positions()
    pairs = [(wide(row), number_above(columns, wide(row))) for row in rows]
    return as_row(placed(pairs, TOPK // 8, sub), sub, twice)


def best_of_block(total_ref, col_ref):
    sub, lane, _ = positions()
    rows = descending([total_ref[k:k + 1, :] for k in range(8)])
    for k, row in enumerate(rows):
        col_ref[k * LANES:(k + 1) * LANES, :] = column_of(row)
    kept = []
    for k, row in enumerate(rows):
        columns = [col_ref[k * LANES + 8 * j:k * LANES + 8 * j + 8, :] for j in range(16)]
        above = number_above(columns, wide(row))
        kept += placed([(wide(row), above)], -(-(TOPK // (k + 1)) // 8), sub)
    first = as_row(kept[:16], sub, lane)
    second = jnp.where(lane[:1] < 8.0 * (len(kept) - 16), as_row(kept[16:], sub, lane), -jnp.inf)
    return order_pair([first, second], kept)


def best_of_lists(lists, col_ref):
    lane = lax.broadcasted_iota(jnp.int32, (1, LANES), 1)
    rows = descending(lists)
    low = jnp.full((1, LANES), -jnp.inf, F32)
    packed = []
    for group in ((0, 1, 2, 5), (3, 4) + tuple(range(6, len(rows)))):
        at, line = 0, low
        for s in group:
            count = TOPK // (s + 1)
            moved = rows[s] if at % TOPK == 0 else pltpu.roll(rows[s], at, 1)
            line = jnp.where((lane >= at) & (lane < at + count), moved, line)
            at += count
        packed.append((line, at))
    columns = []
    for k, (line, used) in enumerate(packed):
        col_ref[k * LANES:(k + 1) * LANES, :] = column_of(line)
        columns += [col_ref[k * LANES + 8 * j:k * LANES + 8 * j + 8, :] for j in range(-(-used // 8))]
    return order_pair([line for line, _ in packed], columns)


def kernel(n_pts, n_cand, points_hbm, weights_hbm, cover_hbm, cand_hbm, picks_hbm, *refs):
    gains_refs, ncov_refs, top_ref = refs[:8], refs[8:16], refs[16]
    (
        points, cands, weights, cover, picks, wcol, ccol, bias, maxes, col,
        part_out, part_in, cov_out, cov_in, top_out, top_in, gains,
        in_sem, p_send, p_recv, c_send, c_recv, t_send, t_recv, near_sem,
    ) = refs[17:]
    n = points.shape[0]
    m = cands.shape[0]
    me_p = lax.axis_index("pts")
    me_c = lax.axis_index("cand")

    half = n // 2
    place = [lax.rem(me_p // 8 + k, 4) * 8 for k in range(4)], [lax.rem(me_p // 2 + k, 4) * 2 for k in range(4)]
    cores = lax.rem(me_p, 2), 1 - lax.rem(me_p, 2)
    offsets = [(x, y, c) for x in range(4) for y in range(4) for c in range(2) if x or y or c]
    offsets.sort(key=lambda o: -(min(o[0], 4 - o[0]) + min(o[1], 4 - o[1])))
    far_first = [place[0][x] + place[1][y] + cores[c] for x, y, c in offsets]
    along = sorted(range(1, n_cand), key=lambda k: -min(k, n_cand - k))
    copies = [
        pltpu.make_async_copy(cover_hbm, cover, in_sem.at[0]),
        pltpu.make_async_copy(weights_hbm, weights, in_sem.at[1]),
        pltpu.make_async_copy(picks_hbm, picks, in_sem.at[2]),
        pltpu.make_async_copy(cand_hbm.at[pl.ds(0, m // 2)], cands.at[pl.ds(0, m // 2)], in_sem.at[3]),
        pltpu.make_async_copy(points_hbm.at[pl.ds(0, half)], points.at[pl.ds(0, half)], in_sem.at[4]),
        pltpu.make_async_copy(points_hbm.at[pl.ds(half, half)], points.at[pl.ds(half, half)], in_sem.at[5]),
        pltpu.make_async_copy(cand_hbm.at[pl.ds(m // 2, m // 2)], cands.at[pl.ds(m // 2, m // 2)], in_sem.at[6]),
    ]
    for copy in copies:
        copy.start()

    near = 4
    beside = [k for k in range(1, n_cand) if min(k, n_cand - k) <= near]
    barrier = pltpu.get_barrier_semaphore()
    for peer in far_first:
        pl.semaphore_signal(barrier, 1, device_id={"pts": peer}, device_id_type=pl.DeviceIdType.MESH)
    for k in beside:
        pl.semaphore_signal(barrier, 1, device_id={"cand": lax.rem(me_c + k, n_cand)}, device_id_type=pl.DeviceIdType.MESH)

    copies[0].wait()
    copies[1].wait()
    for k in range(8):
        ccol[k * LANES:(k + 1) * LANES, :] = column_of(cover[k:k + 1, :] * 32.0)
        wcol[k * LANES:(k + 1) * LANES, :] = column_of(weights[k:k + 1, :] * (2.0 ** -20))
    copies[2].wait()
    column = (
        me_c * m
        + lax.broadcasted_iota(jnp.int32, (8, LANES), 0) * LANES
        + lax.broadcasted_iota(jnp.int32, (8, LANES), 1)
    )
    mask = jnp.full((8, LANES), -1e30, F32)
    for k in range(TOPK):
        mask = jnp.where(column == picks[k], 0.0, mask)
    bias[...] = mask
    copies[3].wait()
    copies[4].wait()

    sums = [jnp.zeros((8, LANES), F32) for _ in range(8)]

    def multiply(tile, rows, first):
        at = slice(rows * half, (rows + 1) * half)
        sims = lax.dot_general(
            points[at, :], cands[tile * 256:(tile + 1) * 256, :], (((1,), (1,)), ((), ())), preferred_element_type=F32
        )
        high = None
        for h in range(2):
            s = sims[:, h * LANES:(h + 1) * LANES]
            t = jnp.maximum(s - ccol[at, :], 0.0) * wcol[at, :]
            sums[2 * tile + h] = sums[2 * tile + h] + jnp.sum(t.reshape(half // 8, 8, LANES), axis=0)
            masked = s + bias[2 * tile + h:2 * tile + h + 1, :]
            high = masked if high is None else jnp.maximum(high, masked)
        maxes[at, :] = high if first else jnp.maximum(maxes[at, :], high)

    def send_parts(start, size):
        for k in range(start, start + size):
            part_out[k:k + 1, :] = jnp.sum(sums[k], axis=0, keepdims=True)
        part_in[me_p, start:start + size, :] = part_out[start:start + size, :]
        for peer in far_first:
            pltpu.make_async_remote_copy(
                part_out.at[pl.ds(start, size)], part_in.at[me_p, pl.ds(start, size)], p_send, p_recv,
                device_id={"pts": peer}, device_id_type=pl.DeviceIdType.MESH,
            ).start()

    multiply(0, 0, True)
    multiply(1, 0, False)
    copies[5].wait()
    copies[6].wait()
    multiply(0, 1, True)
    multiply(1, 1, False)
    for tile in (2, 3):
        for rows in (0, 1):
            multiply(tile, rows, False)
    pl.semaphore_wait(barrier, n_pts - 1 + len(beside))
    send_parts(0, 8)
    reach, rounds = near, 0
    while reach < n_cand // 2:
        for k in (reach, n_cand - reach):
            pl.semaphore_signal(
                near_sem.at[rounds], 1, device_id={"cand": lax.rem(me_c + k, n_cand)}, device_id_type=pl.DeviceIdType.MESH
            )
        if rounds == 0:
            for k in range(8):
                high = maxes[k * LANES:(k + 1) * LANES, :].T
                cov_out[k:k + 1, :] = jnp.max(high, axis=0, keepdims=True) * (2.0 ** -5)
        pl.semaphore_wait(near_sem.at[rounds], 2)
        reach, rounds = 2 * reach, rounds + 1
    for k in along:
        pltpu.make_async_remote_copy(
            cov_out, cov_in.at[k], c_send, c_recv,
            device_id={"cand": lax.rem(me_c + k, n_cand)}, device_id_type=pl.DeviceIdType.MESH,
        ).start()

    some = part_in.at[pl.ds(0, n_pts - 1)]
    pltpu.make_async_copy(some, some, p_recv).wait()
    total = part_in[0]
    for k in range(1, n_pts):
        total = total + part_in[k]
    gains[...] = total
    top_out[...] = best_of_block(gains, col)
    for k in along:
        pltpu.make_async_remote_copy(
            top_out, top_in.at[k], t_send, t_recv,
            device_id={"cand": lax.rem(me_c + k, n_cand)}, device_id_type=pl.DeviceIdType.MESH,
        ).start()

    some = cov_in.at[pl.ds(1, n_cand - 1)]
    pltpu.make_async_copy(some, some, c_recv).wait()
    best = jnp.maximum(cover[...], cov_out[...])
    for k in range(1, n_cand):
        best = jnp.maximum(best, cov_in[k])
    for k in range(8):
        gains_refs[k][...] = gains[k:k + 1, :]
        ncov_refs[k][...] = best[k:k + 1, :]

    for sent, sem, count in ((part_in, p_send, n_pts - 1), (cov_in, c_send, n_cand - 1), (top_in, t_send, n_cand - 1)):
        some = sent.at[pl.ds(0, count)]
        pltpu.make_async_copy(some, some, sem).wait()

    some = top_in.at[pl.ds(1, n_cand - 1)]
    pltpu.make_async_copy(some, some, t_recv).wait()
    best = best_of_lists([top_out[...]] + [top_in[k] for k in range(1, n_cand)], col)
    top_ref[...] = best


def write_out(*refs):
    rows, (gains, ncov, top), (best, sem) = refs[:17], refs[17:20], refs[20:]
    best[...] = rows[16][:, :TOPK]
    copies = [pltpu.make_async_copy(best, top, sem.at[16])]
    for k in range(8):
        copies.append(pltpu.make_async_copy(rows[k], gains.at[pl.ds(k, 1)], sem.at[k]))
        copies.append(pltpu.make_async_copy(rows[8 + k], ncov.at[pl.ds(k, 1)], sem.at[8 + k]))
    for copy in copies:
        copy.start()
    for copy in copies:
        copy.wait()


def on_device(points, weights, coverage, candidates, picks):
    n_pts, n_cand = lax.axis_size("pts"), lax.axis_size("cand")
    n, d = points.shape
    m = candidates.shape[0]
    hbm = pl.BlockSpec(memory_space=pl.ANY)
    vmem = pl.BlockSpec(memory_space=pltpu.VMEM)
    dma = pltpu.SemaphoreType.DMA
    inside = pl.pallas_call(
        functools.partial(kernel, n_pts, n_cand),
        out_shape=(jax.ShapeDtypeStruct((1, LANES), F32),) * 17,
        in_specs=[hbm] * 5,
        out_specs=(vmem,) * 17,
        scratch_shapes=[
            pltpu.VMEM((n, d), jnp.bfloat16),
            pltpu.VMEM((m, d), jnp.bfloat16),
            pltpu.VMEM((8, LANES), F32),
            pltpu.VMEM((8, LANES), F32),
            pltpu.SMEM((TOPK,), jnp.int32),
            pltpu.VMEM((n, LANES), F32),
            pltpu.VMEM((n, LANES), F32),
            pltpu.VMEM((8, LANES), F32),
            pltpu.VMEM((n, LANES), F32),
            pltpu.VMEM((1024, LANES), F32),
            pltpu.VMEM((8, LANES), F32),
            pltpu.VMEM((n_pts, 8, LANES), F32),
            pltpu.VMEM((8, LANES), F32),
            pltpu.VMEM((n_cand, 8, LANES), F32),
            pltpu.VMEM((1, LANES), F32),
            pltpu.VMEM((n_cand, 1, LANES), F32),
            pltpu.VMEM((8, LANES), F32),
            dma((7,)), dma, dma, dma, dma, dma, dma, pltpu.SemaphoreType.REGULAR((1,)),
        ],
        compiler_params=pltpu.CompilerParams(
            collective_id=0, has_side_effects=True, vmem_limit_bytes=VMEM_BYTES
        ),
        name="facility",
    )(points, weights.reshape(8, LANES), coverage.reshape(8, LANES), candidates, picks)
    gains, ncov, top = pl.pallas_call(
        write_out,
        out_shape=(
            jax.ShapeDtypeStruct((8, LANES), F32),
            jax.ShapeDtypeStruct((8, LANES), F32),
            jax.ShapeDtypeStruct((1, TOPK), F32),
        ),
        in_specs=[vmem] * 17,
        out_specs=(hbm, hbm, hbm),
        scratch_shapes=[pltpu.VMEM((1, TOPK), F32), dma((17,))],
        compiler_params=pltpu.CompilerParams(vmem_limit_bytes=2**20),
        name="write_out",
    )(*inside)
    return gains.reshape(m), top.reshape(TOPK), ncov.reshape(n)


def solution(mesh):
    placed = (P("pts", None), P("pts"), P("pts"), P("cand", None), P())
    return jax.shard_map(
        on_device, mesh=mesh, in_specs=placed, out_specs=(P("cand"), P(), P("pts")), check_vma=False
    )
```

```python
import functools

import jax
import jax.numpy as jnp
from jax import lax
from jax.experimental import pallas as pl
from jax.experimental.pallas import tpu as pltpu
from jax.sharding import PartitionSpec as P

TOPK = 64
LANES = 128
F32 = jnp.float32
VMEM_BYTES = 56557568 - 70 * 1024


def column_of(row):
    return jnp.broadcast_to(row, (LANES, LANES)).T


def descending(rows):
    rows, n, p = list(rows), len(rows), 1
    while p < n:
        k = p
        while k >= 1:
            for j in range(k % p, n - k, 2 * k):
                for i in range(min(k, n - j - k)):
                    if (i + j) // (2 * p) == (i + j + k) // (2 * p):
                        x, y = rows[i + j], rows[i + j + k]
                        rows[i + j], rows[i + j + k] = jnp.maximum(x, y), jnp.minimum(x, y)
            k //= 2
        p *= 2
    return rows


def wide(row):
    return jnp.broadcast_to(row, (8, LANES))


def added(terms):
    while len(terms) > 1:
        terms = [x + y for x, y in zip(terms[::2], terms[1::2])] + ([terms[-1]] if len(terms) % 2 else [])
    return terms[0]


def number_above(columns, row):
    total = added([jnp.where(column > row, 1.0, 0.0) for column in columns])
    return wide(jnp.sum(total, axis=0, keepdims=True))


def placed(pairs, blocks, sub):
    result = []
    for block in range(blocks):
        place = sub + float(block * 8)
        best = jnp.full((8, LANES), jnp.inf, F32)
        for row, above in pairs:
            best = jnp.minimum(best, jnp.where(above <= place, row, jnp.inf))
        result.append(jnp.broadcast_to(jnp.min(best, axis=1, keepdims=True), (8, LANES)))
    return result


def as_row(blocks, sub, lane):
    total = added([jnp.where(lane == sub + float(index * 8), block, 0.0) for index, block in enumerate(blocks)])
    return jnp.sum(total, axis=0, keepdims=True)


def positions():
    sub = lax.broadcasted_iota(jnp.int32, (8, LANES), 0).astype(F32)
    lane = lax.broadcasted_iota(jnp.int32, (8, LANES), 1)
    return sub, lane.astype(F32), lax.rem(lane, TOPK).astype(F32)


def order_pair(rows, columns):
    sub, _, twice = positions()
    pairs = [(wide(row), number_above(columns, wide(row))) for row in rows]
    return as_row(placed(pairs, TOPK // 8, sub), sub, twice)


def best_of_block(total_ref, col_ref):
    sub, lane, _ = positions()
    rows = descending([total_ref[k:k + 1, :] for k in range(8)])
    for k, row in enumerate(rows):
        col_ref[k * LANES:(k + 1) * LANES, :] = column_of(row)
    kept = []
    for k, row in enumerate(rows):
        columns = [col_ref[k * LANES + 8 * j:k * LANES + 8 * j + 8, :] for j in range(16)]
        above = number_above(columns, wide(row))
        kept += placed([(wide(row), above)], -(-(TOPK // (k + 1)) // 8), sub)
    first = as_row(kept[:16], sub, lane)
    second = jnp.where(lane[:1] < 8.0 * (len(kept) - 16), as_row(kept[16:], sub, lane), -jnp.inf)
    return order_pair([first, second], kept)


def best_of_lists(lists, col_ref):
    lane = lax.broadcasted_iota(jnp.int32, (1, LANES), 1)
    rows = descending(lists)
    low = jnp.full((1, LANES), -jnp.inf, F32)
    packed = []
    for group in ((0, 1, 2, 5), (3, 4) + tuple(range(6, len(rows)))):
        at, line = 0, low
        for s in group:
            if s < len(rows):
                count = TOPK // (s + 1)
                moved = rows[s] if at % TOPK == 0 else pltpu.roll(rows[s], at, 1)
                line = jnp.where((lane >= at) & (lane < at + count), moved, line)
                at += count
        if at:
            packed.append((line, at))
    columns = []
    for k, (line, used) in enumerate(packed):
        col_ref[k * LANES:(k + 1) * LANES, :] = column_of(line)
        columns += [col_ref[k * LANES + 8 * j:k * LANES + 8 * j + 8, :] for j in range(-(-used // 8))]
    return order_pair([line for line, _ in packed], columns)


def kernel(n_pts, n_cand, points_hbm, weights_hbm, cover_hbm, cand_hbm, picks_hbm, *refs):
    gains_refs, ncov_refs, top_ref = refs[:8], refs[8:16], refs[16]
    (
        points, cands, weights, cover, picks, wcol, ccol, bias, maxes, col,
        part_out, part_in, cov_out, cov_in, top_out, top_in, gains,
        in_sem, p_send, p_recv, c_send, c_recv, t_send, t_recv, near_sem,
    ) = refs[17:]
    n = points.shape[0]
    m = cands.shape[0]
    me_p = lax.axis_index("pts")
    me_c = lax.axis_index("cand")

    half = n // 2
    place = [lax.rem(me_p // 8 + k, 4) * 8 for k in range(4)], [lax.rem(me_p // 2 + k, 4) * 2 for k in range(4)]
    cores = lax.rem(me_p, 2), 1 - lax.rem(me_p, 2)
    offsets = [(x, y, c) for x in range(4) for y in range(4) for c in range(2) if x or y or c]
    offsets.sort(key=lambda o: -(min(o[0], 4 - o[0]) + min(o[1], 4 - o[1])))
    far_first = [place[0][x] + place[1][y] + cores[c] for x, y, c in offsets]
    farthest = n_cand // 2
    along = sorted(range(1, n_cand), key=lambda k: -min(k, n_cand - k))
    copies = [
        pltpu.make_async_copy(cover_hbm, cover, in_sem.at[0]),
        pltpu.make_async_copy(weights_hbm, weights, in_sem.at[1]),
        pltpu.make_async_copy(picks_hbm, picks, in_sem.at[2]),
        pltpu.make_async_copy(cand_hbm.at[pl.ds(0, m // 2)], cands.at[pl.ds(0, m // 2)], in_sem.at[3]),
        pltpu.make_async_copy(points_hbm.at[pl.ds(0, half)], points.at[pl.ds(0, half)], in_sem.at[4]),
        pltpu.make_async_copy(points_hbm.at[pl.ds(half, half)], points.at[pl.ds(half, half)], in_sem.at[5]),
        pltpu.make_async_copy(cand_hbm.at[pl.ds(m // 2, m // 2)], cands.at[pl.ds(m // 2, m // 2)], in_sem.at[6]),
    ]
    for copy in copies:
        copy.start()

    near = 4
    beside = [k for k in range(1, n_cand) if min(k, n_cand - k) <= near]
    barrier = pltpu.get_barrier_semaphore()
    for peer in far_first:
        pl.semaphore_signal(barrier, 1, device_id={"pts": peer}, device_id_type=pl.DeviceIdType.MESH)
    for k in beside:
        pl.semaphore_signal(barrier, 1, device_id={"cand": lax.rem(me_c + k, n_cand)}, device_id_type=pl.DeviceIdType.MESH)

    copies[0].wait()
    copies[1].wait()
    for k in range(8):
        ccol[k * LANES:(k + 1) * LANES, :] = column_of(cover[k:k + 1, :] * 32.0)
        wcol[k * LANES:(k + 1) * LANES, :] = column_of(weights[k:k + 1, :] * (2.0 ** -20))
    copies[2].wait()
    column = (
        me_c * m
        + lax.broadcasted_iota(jnp.int32, (8, LANES), 0) * LANES
        + lax.broadcasted_iota(jnp.int32, (8, LANES), 1)
    )
    mask = jnp.full((8, LANES), -1e30, F32)
    for k in range(TOPK):
        mask = jnp.where(column == picks[k], 0.0, mask)
    bias[...] = mask
    copies[3].wait()
    copies[4].wait()

    sums = [jnp.zeros((8, LANES), F32) for _ in range(8)]

    def multiply(tile, rows, first):
        at = slice(rows * half, (rows + 1) * half)
        sims = lax.dot_general(
            points[at, :], cands[tile * 256:(tile + 1) * 256, :], (((1,), (1,)), ((), ())), preferred_element_type=F32
        )
        high = None
        for h in range(2):
            s = sims[:, h * LANES:(h + 1) * LANES]
            t = jnp.maximum(s - ccol[at, :], 0.0) * wcol[at, :]
            sums[2 * tile + h] = sums[2 * tile + h] + jnp.sum(t.reshape(half // 8, 8, LANES), axis=0)
            masked = s + bias[2 * tile + h:2 * tile + h + 1, :]
            high = masked if high is None else jnp.maximum(high, masked)
        maxes[at, :] = high if first else jnp.maximum(maxes[at, :], high)

    def send_parts(start, size):
        for k in range(start, start + size):
            part_out[k:k + 1, :] = jnp.sum(sums[k], axis=0, keepdims=True)
        part_in[me_p, start:start + size, :] = part_out[start:start + size, :]
        for peer in far_first:
            pltpu.make_async_remote_copy(
                part_out.at[pl.ds(start, size)], part_in.at[me_p, pl.ds(start, size)], p_send, p_recv,
                device_id={"pts": peer}, device_id_type=pl.DeviceIdType.MESH,
            ).start()

    multiply(0, 0, True)
    multiply(1, 0, False)
    copies[5].wait()
    copies[6].wait()
    multiply(0, 1, True)
    multiply(1, 1, False)
    for tile in (2, 3):
        for rows in (0, 1):
            multiply(tile, rows, False)
    pl.semaphore_wait(barrier, n_pts - 1 + len(beside))
    send_parts(0, 8)
    reach, rounds = near, 0
    while reach < n_cand // 2:
        for k in (reach, n_cand - reach):
            pl.semaphore_signal(
                near_sem.at[rounds], 1, device_id={"cand": lax.rem(me_c + k, n_cand)}, device_id_type=pl.DeviceIdType.MESH
            )
        if rounds == 0:
            for k in range(8):
                high = maxes[k * LANES:(k + 1) * LANES, :].T
                cov_out[k:k + 1, :] = jnp.max(high, axis=0, keepdims=True) * (2.0 ** -5)
        pl.semaphore_wait(near_sem.at[rounds], 2)
        reach, rounds = 2 * reach, rounds + 1
    for k in along:
        pltpu.make_async_remote_copy(
            cov_out, cov_in.at[k], c_send, c_recv,
            device_id={"cand": lax.rem(me_c + k, n_cand)}, device_id_type=pl.DeviceIdType.MESH,
        ).start()

    some = part_in.at[pl.ds(0, n_pts - 1)]
    pltpu.make_async_copy(some, some, p_recv).wait()
    total = part_in[0]
    for k in range(1, n_pts):
        total = total + part_in[k]
    gains[...] = total
    top_out[...] = best_of_block(gains, col)
    for k in along:
        pltpu.make_async_remote_copy(
            top_out, top_in.at[k], t_send, t_recv.at[int(k == farthest)],
            device_id={"cand": lax.rem(me_c + k, n_cand)}, device_id_type=pl.DeviceIdType.MESH,
        ).start()

    some = cov_in.at[pl.ds(1, n_cand - 1)]
    pltpu.make_async_copy(some, some, c_recv).wait()
    best = jnp.maximum(cover[...], cov_out[...])
    for k in range(1, n_cand):
        best = jnp.maximum(best, cov_in[k])
    for k in range(8):
        gains_refs[k][...] = gains[k:k + 1, :]
        ncov_refs[k][...] = best[k:k + 1, :]

    some = top_in.at[pl.ds(0, n_cand - 2)]
    pltpu.make_async_copy(some, some, t_recv.at[0]).wait()
    best = best_of_lists([top_out[...]] + [top_in[k] for k in range(1, n_cand) if k != farthest], col)

    for sent, sem, count in ((part_in, p_send, n_pts - 1), (cov_in, c_send, n_cand - 1), (top_in, t_send, n_cand - 1)):
        some = sent.at[pl.ds(0, count)]
        pltpu.make_async_copy(some, some, sem).wait()

    some = top_in.at[pl.ds(farthest, 1)]
    pltpu.make_async_copy(some, some, t_recv.at[1]).wait()
    top_ref[...] = best_of_lists([best, top_in[farthest]], col)


def write_out(*refs):
    rows, (gains, ncov, top), (gains_all, ncov_all, best, sem) = refs[:17], refs[17:20], refs[20:]
    best[...] = rows[16][:, :TOPK]
    for k in range(8):
        gains_all[k:k + 1, :] = rows[k][...]
        ncov_all[k:k + 1, :] = rows[8 + k][...]
    copies = [
        pltpu.make_async_copy(best, top, sem.at[0]),
        pltpu.make_async_copy(gains_all, gains, sem.at[1]),
        pltpu.make_async_copy(ncov_all, ncov, sem.at[2]),
    ]
    for copy in copies:
        copy.start()
    for copy in copies:
        copy.wait()


def on_device(points, weights, coverage, candidates, picks):
    n_pts, n_cand = lax.axis_size("pts"), lax.axis_size("cand")
    n, d = points.shape
    m = candidates.shape[0]
    hbm = pl.BlockSpec(memory_space=pl.ANY)
    vmem = pl.BlockSpec(memory_space=pltpu.VMEM)
    dma = pltpu.SemaphoreType.DMA
    inside = pl.pallas_call(
        functools.partial(kernel, n_pts, n_cand),
        out_shape=(jax.ShapeDtypeStruct((1, LANES), F32),) * 17,
        in_specs=[hbm] * 5,
        out_specs=(vmem,) * 17,
        scratch_shapes=[
            pltpu.VMEM((n, d), jnp.bfloat16),
            pltpu.VMEM((m, d), jnp.bfloat16),
            pltpu.VMEM((8, LANES), F32),
            pltpu.VMEM((8, LANES), F32),
            pltpu.SMEM((TOPK,), jnp.int32),
            pltpu.VMEM((n, LANES), F32),
            pltpu.VMEM((n, LANES), F32),
            pltpu.VMEM((8, LANES), F32),
            pltpu.VMEM((n, LANES), F32),
            pltpu.VMEM((1024, LANES), F32),
            pltpu.VMEM((8, LANES), F32),
            pltpu.VMEM((n_pts, 8, LANES), F32),
            pltpu.VMEM((8, LANES), F32),
            pltpu.VMEM((n_cand, 8, LANES), F32),
            pltpu.VMEM((1, LANES), F32),
            pltpu.VMEM((n_cand, 1, LANES), F32),
            pltpu.VMEM((8, LANES), F32),
            dma((7,)), dma, dma, dma, dma, dma, dma((2,)), pltpu.SemaphoreType.REGULAR((1,)),
        ],
        compiler_params=pltpu.CompilerParams(
            collective_id=0, has_side_effects=True, vmem_limit_bytes=VMEM_BYTES
        ),
        name="facility",
    )(points, weights.reshape(8, LANES), coverage.reshape(8, LANES), candidates, picks)
    gains, ncov, top = pl.pallas_call(
        write_out,
        out_shape=(
            jax.ShapeDtypeStruct((8, LANES), F32),
            jax.ShapeDtypeStruct((8, LANES), F32),
            jax.ShapeDtypeStruct((1, TOPK), F32),
        ),
        in_specs=[vmem] * 17,
        out_specs=(hbm, hbm, hbm),
        scratch_shapes=[
            pltpu.VMEM((8, LANES), F32), pltpu.VMEM((8, LANES), F32), pltpu.VMEM((1, TOPK), F32), dma((3,))
        ],
        compiler_params=pltpu.CompilerParams(vmem_limit_bytes=2**20),
        name="write_out",
    )(*inside)
    return gains.reshape(m), top.reshape(TOPK), ncov.reshape(n)


def solution(mesh):
    placed = (P("pts", None), P("pts"), P("pts"), P("cand", None), P())
    return jax.shard_map(
        on_device, mesh=mesh, in_specs=placed, out_specs=(P("cand"), P(), P("pts")), check_vma=False
    )
```

```python
import functools

import jax
import jax.numpy as jnp
from jax import lax
from jax.experimental import pallas as pl
from jax.experimental.pallas import tpu as pltpu
from jax.sharding import PartitionSpec as P

TOPK = 64
LANES = 128
F32 = jnp.float32
VMEM_BYTES = 56557568 - 70 * 1024


def column_of(row):
    return jnp.broadcast_to(row, (LANES, LANES)).T


def descending(rows):
    rows, n, p = list(rows), len(rows), 1
    while p < n:
        k = p
        while k >= 1:
            for j in range(k % p, n - k, 2 * k):
                for i in range(min(k, n - j - k)):
                    if (i + j) // (2 * p) == (i + j + k) // (2 * p):
                        x, y = rows[i + j], rows[i + j + k]
                        rows[i + j], rows[i + j + k] = jnp.maximum(x, y), jnp.minimum(x, y)
            k //= 2
        p *= 2
    return rows


def wide(row):
    return jnp.broadcast_to(row, (8, LANES))


def added(terms):
    while len(terms) > 1:
        terms = [x + y for x, y in zip(terms[::2], terms[1::2])] + ([terms[-1]] if len(terms) % 2 else [])
    return terms[0]


def number_above(columns, row):
    total = added([jnp.where(column > row, 1.0, 0.0) for column in columns])
    return wide(jnp.sum(total, axis=0, keepdims=True))


def placed(pairs, blocks, sub):
    result = []
    for block in range(blocks):
        place = sub + float(block * 8)
        best = jnp.full((8, LANES), jnp.inf, F32)
        for row, above in pairs:
            best = jnp.minimum(best, jnp.where(above <= place, row, jnp.inf))
        result.append(jnp.broadcast_to(jnp.min(best, axis=1, keepdims=True), (8, LANES)))
    return result


def as_row(blocks, sub, lane):
    total = added([jnp.where(lane == sub + float(index * 8), block, 0.0) for index, block in enumerate(blocks)])
    return jnp.sum(total, axis=0, keepdims=True)


def positions():
    sub = lax.broadcasted_iota(jnp.int32, (8, LANES), 0).astype(F32)
    lane = lax.broadcasted_iota(jnp.int32, (8, LANES), 1)
    return sub, lane.astype(F32), lax.rem(lane, TOPK).astype(F32)


def order_pair(rows, columns):
    sub, _, twice = positions()
    pairs = [(wide(row), number_above(columns, wide(row))) for row in rows]
    return as_row(placed(pairs, TOPK // 8, sub), sub, twice)


def best_of_block(total_ref, col_ref):
    sub, lane, _ = positions()
    rows = descending([total_ref[k:k + 1, :] for k in range(8)])
    for k, row in enumerate(rows):
        col_ref[k * LANES:(k + 1) * LANES, :] = column_of(row)
    kept = []
    for k, row in enumerate(rows):
        columns = [col_ref[k * LANES + 8 * j:k * LANES + 8 * j + 8, :] for j in range(16)]
        above = number_above(columns, wide(row))
        kept += placed([(wide(row), above)], -(-(TOPK // (k + 1)) // 8), sub)
    first = as_row(kept[:16], sub, lane)
    second = jnp.where(lane[:1] < 8.0 * (len(kept) - 16), as_row(kept[16:], sub, lane), -jnp.inf)
    return order_pair([first, second], kept)


def best_of_lists(lists, col_ref):
    lane = lax.broadcasted_iota(jnp.int32, (1, LANES), 1)
    rows = descending(lists)
    low = jnp.full((1, LANES), -jnp.inf, F32)
    packed = []
    for group in ((0, 1, 2, 5), (3, 4) + tuple(range(6, len(rows)))):
        at, line = 0, low
        for s in group:
            if s < len(rows):
                count = TOPK // (s + 1)
                moved = rows[s] if at % TOPK == 0 else pltpu.roll(rows[s], at, 1)
                line = jnp.where((lane >= at) & (lane < at + count), moved, line)
                at += count
        if at:
            packed.append((line, at))
    columns = []
    for k, (line, used) in enumerate(packed):
        col_ref[k * LANES:(k + 1) * LANES, :] = column_of(line)
        columns += [col_ref[k * LANES + 8 * j:k * LANES + 8 * j + 8, :] for j in range(-(-used // 8))]
    return order_pair([line for line, _ in packed], columns)


def kernel(n_pts, n_cand, points_hbm, weights_hbm, cover_hbm, cand_hbm, picks_hbm, *refs):
    gains_refs, ncov_refs, top_ref = refs[:8], refs[8:16], refs[16]
    (
        points, cands, weights, cover, picks, wcol, ccol, bias, maxes, col,
        part_out, part_in, cov_out, cov_in, top_out, top_in, top_near, gains,
        p_recv, c_recv, t_recv, near_sem,
    ) = refs[17:]
    farthest = n_cand // 2

    def until_last_list(in_sem, p_send, c_send, t_send):
        n = points.shape[0]
        m = cands.shape[0]
        me_p = lax.axis_index("pts")
        me_c = lax.axis_index("cand")

        half = n // 2
        others = [k + lax.div(k - me_p + n_pts - 1, n_pts - 1) for k in range(n_pts - 1)]
        along = sorted(range(1, n_cand), key=lambda k: -min(k, n_cand - k))
        copies = [
            pltpu.make_async_copy(cover_hbm, cover, in_sem.at[0]),
            pltpu.make_async_copy(weights_hbm, weights, in_sem.at[1]),
            pltpu.make_async_copy(picks_hbm, picks, in_sem.at[2]),
            pltpu.make_async_copy(cand_hbm.at[pl.ds(0, m // 2)], cands.at[pl.ds(0, m // 2)], in_sem.at[3]),
            pltpu.make_async_copy(points_hbm.at[pl.ds(0, half)], points.at[pl.ds(0, half)], in_sem.at[4]),
            pltpu.make_async_copy(points_hbm.at[pl.ds(half, half)], points.at[pl.ds(half, half)], in_sem.at[5]),
            pltpu.make_async_copy(cand_hbm.at[pl.ds(m // 2, m // 2)], cands.at[pl.ds(m // 2, m // 2)], in_sem.at[6]),
        ]
        for copy in copies:
            copy.start()

        near = 4
        beside = [k for k in range(1, n_cand) if min(k, n_cand - k) <= near]
        barrier = pltpu.get_barrier_semaphore()
        for peer in others:
            pl.semaphore_signal(barrier, 1, device_id={"pts": peer}, device_id_type=pl.DeviceIdType.MESH)
        for k in beside:
            pl.semaphore_signal(barrier, 1, device_id={"cand": lax.rem(me_c + k, n_cand)}, device_id_type=pl.DeviceIdType.MESH)

        copies[0].wait()
        copies[1].wait()
        for k in range(8):
            ccol[k * LANES:(k + 1) * LANES, :] = column_of(cover[k:k + 1, :] * 32.0)
            wcol[k * LANES:(k + 1) * LANES, :] = column_of(weights[k:k + 1, :] * (2.0 ** -20))
        copies[2].wait()
        column = (
            me_c * m
            + lax.broadcasted_iota(jnp.int32, (8, LANES), 0) * LANES
            + lax.broadcasted_iota(jnp.int32, (8, LANES), 1)
        )
        mask = jnp.full((8, LANES), -1e30, F32)
        for k in range(TOPK):
            mask = jnp.where(column == picks[k], 0.0, mask)
        bias[...] = mask
        copies[3].wait()
        copies[4].wait()

        sums = [jnp.zeros((8, LANES), F32) for _ in range(8)]

        def multiply(tile, rows, first):
            at = slice(rows * half, (rows + 1) * half)
            sims = lax.dot_general(
                points[at, :], cands[tile * 256:(tile + 1) * 256, :], (((1,), (1,)), ((), ())), preferred_element_type=F32
            )
            high = None
            for h in range(2):
                s = sims[:, h * LANES:(h + 1) * LANES]
                t = jnp.maximum(s - ccol[at, :], 0.0) * wcol[at, :]
                sums[2 * tile + h] = sums[2 * tile + h] + jnp.sum(t.reshape(half // 8, 8, LANES), axis=0)
                masked = s + bias[2 * tile + h:2 * tile + h + 1, :]
                high = masked if high is None else jnp.maximum(high, masked)
            maxes[at, :] = high if first else jnp.maximum(maxes[at, :], high)

        def send_parts(start, size):
            for k in range(start, start + size):
                part_out[k:k + 1, :] = jnp.sum(sums[k], axis=0, keepdims=True)
            part_in[me_p, start:start + size, :] = part_out[start:start + size, :]
            for peer in others:
                pltpu.make_async_remote_copy(
                    part_out.at[pl.ds(start, size)], part_in.at[me_p, pl.ds(start, size)], p_send, p_recv,
                    device_id={"pts": peer}, device_id_type=pl.DeviceIdType.MESH,
                ).start()

        multiply(0, 0, True)
        multiply(1, 0, False)
        copies[5].wait()
        copies[6].wait()
        multiply(0, 1, True)
        multiply(1, 1, False)
        for tile in (2, 3):
            for rows in (0, 1):
                multiply(tile, rows, False)
        pl.semaphore_wait(barrier, n_pts - 1 + len(beside))
        send_parts(0, 8)
        reach, rounds = near, 0
        while reach < n_cand // 2:
            for k in (reach, n_cand - reach):
                pl.semaphore_signal(
                    near_sem.at[rounds], 1, device_id={"cand": lax.rem(me_c + k, n_cand)}, device_id_type=pl.DeviceIdType.MESH
                )
            if rounds == 0:
                for k in range(8):
                    high = maxes[k * LANES:(k + 1) * LANES, :].T
                    cov_out[k:k + 1, :] = jnp.max(high, axis=0, keepdims=True) * (2.0 ** -5)
            pl.semaphore_wait(near_sem.at[rounds], 2)
            reach, rounds = 2 * reach, rounds + 1
        for k in along:
            pltpu.make_async_remote_copy(
                cov_out, cov_in.at[k], c_send, c_recv,
                device_id={"cand": lax.rem(me_c + k, n_cand)}, device_id_type=pl.DeviceIdType.MESH,
            ).start()

        some = part_in.at[pl.ds(0, n_pts - 1)]
        pltpu.make_async_copy(some, some, p_recv).wait()
        total = part_in[0]
        for k in range(1, n_pts):
            total = total + part_in[k]
        gains[...] = total
        top_out[...] = best_of_block(gains, col)
        for k in along:
            pltpu.make_async_remote_copy(
                top_out, top_in.at[k], t_send, t_recv.at[int(k == farthest)],
                device_id={"cand": lax.rem(me_c + k, n_cand)}, device_id_type=pl.DeviceIdType.MESH,
            ).start()

        some = cov_in.at[pl.ds(1, n_cand - 1)]
        pltpu.make_async_copy(some, some, c_recv).wait()
        best = jnp.maximum(cover[...], cov_out[...])
        for k in range(1, n_cand):
            best = jnp.maximum(best, cov_in[k])
        for k in range(8):
            gains_refs[k][...] = gains[k:k + 1, :]
            ncov_refs[k][...] = best[k:k + 1, :]

        some = top_in.at[pl.ds(0, n_cand - 2)]
        pltpu.make_async_copy(some, some, t_recv.at[0]).wait()
        top_near[...] = best_of_lists([top_out[...]] + [top_in[k] for k in range(1, n_cand) if k != farthest], col)

        for sent, sem, count in ((part_in, p_send, n_pts - 1), (cov_in, c_send, n_cand - 1), (top_in, t_send, n_cand - 1)):
            some = sent.at[pl.ds(0, count)]
            pltpu.make_async_copy(some, some, sem).wait()

    dma = pltpu.SemaphoreType.DMA
    pl.run_scoped(until_last_list, dma((7,)), dma, dma, dma)

    some = top_in.at[pl.ds(farthest, 1)]
    pltpu.make_async_copy(some, some, t_recv.at[1]).wait()
    top_ref[...] = best_of_lists([top_near[...], top_in[farthest]], col)


def write_out(*refs):
    rows, (gains, ncov, top), (gains_all, ncov_all, best, sem) = refs[:17], refs[17:20], refs[20:]
    best[...] = rows[16][:, :TOPK]
    for k in range(8):
        gains_all[k:k + 1, :] = rows[k][...]
        ncov_all[k:k + 1, :] = rows[8 + k][...]
    copies = [
        pltpu.make_async_copy(best, top, sem.at[0]),
        pltpu.make_async_copy(gains_all, gains, sem.at[1]),
        pltpu.make_async_copy(ncov_all, ncov, sem.at[2]),
    ]
    for copy in copies:
        copy.start()
    for copy in copies:
        copy.wait()


def on_device(points, weights, coverage, candidates, picks):
    n_pts, n_cand = lax.axis_size("pts"), lax.axis_size("cand")
    n, d = points.shape
    m = candidates.shape[0]
    hbm = pl.BlockSpec(memory_space=pl.ANY)
    vmem = pl.BlockSpec(memory_space=pltpu.VMEM)
    dma = pltpu.SemaphoreType.DMA
    inside = pl.pallas_call(
        functools.partial(kernel, n_pts, n_cand),
        out_shape=(jax.ShapeDtypeStruct((1, LANES), F32),) * 17,
        in_specs=[hbm] * 5,
        out_specs=(vmem,) * 17,
        scratch_shapes=[
            pltpu.VMEM((n, d), jnp.bfloat16),
            pltpu.VMEM((m, d), jnp.bfloat16),
            pltpu.VMEM((8, LANES), F32),
            pltpu.VMEM((8, LANES), F32),
            pltpu.SMEM((TOPK,), jnp.int32),
            pltpu.VMEM((n, LANES), F32),
            pltpu.VMEM((n, LANES), F32),
            pltpu.VMEM((8, LANES), F32),
            pltpu.VMEM((n, LANES), F32),
            pltpu.VMEM((1024, LANES), F32),
            pltpu.VMEM((8, LANES), F32),
            pltpu.VMEM((n_pts, 8, LANES), F32),
            pltpu.VMEM((8, LANES), F32),
            pltpu.VMEM((n_cand, 8, LANES), F32),
            pltpu.VMEM((1, LANES), F32),
            pltpu.VMEM((n_cand, 1, LANES), F32),
            pltpu.VMEM((1, LANES), F32),
            pltpu.VMEM((8, LANES), F32),
            dma, dma, dma((2,)), pltpu.SemaphoreType.REGULAR((1,)),
        ],
        compiler_params=pltpu.CompilerParams(
            collective_id=0, has_side_effects=True, vmem_limit_bytes=VMEM_BYTES
        ),
        name="facility",
    )(points, weights.reshape(8, LANES), coverage.reshape(8, LANES), candidates, picks)
    gains, ncov, top = pl.pallas_call(
        write_out,
        out_shape=(
            jax.ShapeDtypeStruct((8, LANES), F32),
            jax.ShapeDtypeStruct((8, LANES), F32),
            jax.ShapeDtypeStruct((1, TOPK), F32),
        ),
        in_specs=[vmem] * 17,
        out_specs=(hbm, hbm, hbm),
        scratch_shapes=[
            pltpu.VMEM((8, LANES), F32), pltpu.VMEM((8, LANES), F32), pltpu.VMEM((1, TOPK), F32), dma((3,))
        ],
        compiler_params=pltpu.CompilerParams(vmem_limit_bytes=2**20),
        name="write_out",
    )(*inside)
    return gains.reshape(m), top.reshape(TOPK), ncov.reshape(n)


def solution(mesh):
    placed = (P("pts", None), P("pts"), P("pts"), P("cand", None), P())
    return jax.shard_map(
        on_device, mesh=mesh, in_specs=placed, out_specs=(P("cand"), P(), P("pts")), check_vma=False
    )
```

```python
import functools

import jax
import jax.numpy as jnp
from jax import lax
from jax.experimental import pallas as pl
from jax.experimental.pallas import tpu as pltpu
from jax.sharding import PartitionSpec as P

TOPK = 64
LANES = 128
F32 = jnp.float32
VMEM_BYTES = 56557568 - 70 * 1024


def column_of(row):
    return jnp.broadcast_to(row, (LANES, LANES)).T


def descending(rows):
    rows, n, p = list(rows), len(rows), 1
    while p < n:
        k = p
        while k >= 1:
            for j in range(k % p, n - k, 2 * k):
                for i in range(min(k, n - j - k)):
                    if (i + j) // (2 * p) == (i + j + k) // (2 * p):
                        x, y = rows[i + j], rows[i + j + k]
                        rows[i + j], rows[i + j + k] = jnp.maximum(x, y), jnp.minimum(x, y)
            k //= 2
        p *= 2
    return rows


def wide(row):
    return jnp.broadcast_to(row, (8, LANES))


def added(terms):
    while len(terms) > 1:
        terms = [x + y for x, y in zip(terms[::2], terms[1::2])] + ([terms[-1]] if len(terms) % 2 else [])
    return terms[0]


def number_above(columns, row):
    total = added([jnp.where(column > row, 1.0, 0.0) for column in columns])
    return wide(jnp.sum(total, axis=0, keepdims=True))


def placed(pairs, blocks, sub):
    result = []
    for block in range(blocks):
        place = sub + float(block * 8)
        best = jnp.full((8, LANES), jnp.inf, F32)
        for row, above in pairs:
            best = jnp.minimum(best, jnp.where(above <= place, row, jnp.inf))
        result.append(jnp.broadcast_to(jnp.min(best, axis=1, keepdims=True), (8, LANES)))
    return result


def as_row(blocks, sub, lane):
    total = added([jnp.where(lane == sub + float(index * 8), block, 0.0) for index, block in enumerate(blocks)])
    return jnp.sum(total, axis=0, keepdims=True)


def positions():
    sub = lax.broadcasted_iota(jnp.int32, (8, LANES), 0).astype(F32)
    lane = lax.broadcasted_iota(jnp.int32, (8, LANES), 1)
    return sub, lane.astype(F32), lax.rem(lane, TOPK).astype(F32)


def order_pair(rows, columns):
    sub, _, twice = positions()
    pairs = [(wide(row), number_above(columns, wide(row))) for row in rows]
    return as_row(placed(pairs, TOPK // 8, sub), sub, twice)


def best_of_block(total_ref, col_ref):
    sub, lane, _ = positions()
    rows = descending([total_ref[k:k + 1, :] for k in range(8)])
    for k, row in enumerate(rows):
        col_ref[k * LANES:(k + 1) * LANES, :] = column_of(row)
    kept = []
    for k, row in enumerate(rows):
        columns = [col_ref[k * LANES + 8 * j:k * LANES + 8 * j + 8, :] for j in range(16)]
        above = number_above(columns, wide(row))
        kept += placed([(wide(row), above)], -(-(TOPK // (k + 1)) // 8), sub)
    first = as_row(kept[:16], sub, lane)
    second = jnp.where(lane[:1] < 8.0 * (len(kept) - 16), as_row(kept[16:], sub, lane), -jnp.inf)
    return order_pair([first, second], kept)


def best_of_lists(lists, col_ref):
    lane = lax.broadcasted_iota(jnp.int32, (1, LANES), 1)
    rows = descending(lists)
    low = jnp.full((1, LANES), -jnp.inf, F32)
    packed = []
    for group in ((0, 1, 2, 5), (3, 4) + tuple(range(6, len(rows)))):
        at, line = 0, low
        for s in group:
            if s < len(rows):
                count = TOPK // (s + 1)
                moved = rows[s] if at % TOPK == 0 else pltpu.roll(rows[s], at, 1)
                line = jnp.where((lane >= at) & (lane < at + count), moved, line)
                at += count
        if at:
            packed.append((line, at))
    columns = []
    for k, (line, used) in enumerate(packed):
        col_ref[k * LANES:(k + 1) * LANES, :] = column_of(line)
        columns += [col_ref[k * LANES + 8 * j:k * LANES + 8 * j + 8, :] for j in range(-(-used // 8))]
    return order_pair([line for line, _ in packed], columns)


def kernel(n_pts, n_cand, points_hbm, weights_hbm, cover_hbm, cand_hbm, picks_hbm, *refs):
    gains_refs, ncov_refs, top_ref = refs[:8], refs[8:16], refs[16]
    (
        points, cands, weights, cover, picks, wcol, ccol, bias, maxes, col,
        part_out, part_in, cov_out, cov_in, top_out, top_in, top_near, gains,
        p_recv, c_recv, t_recv, near_sem,
    ) = refs[17:]
    farthest = n_cand // 2

    def until_last_list(in_sem, p_send, c_send, t_send, *results):
        n, d = points.shape
        m = cands.shape[0]
        me_p = lax.axis_index("pts")
        me_c = lax.axis_index("cand")

        half = n // 2
        along = sorted(range(1, n_cand), key=lambda k: -min(k, n_cand - k))
        copies = [
            pltpu.make_async_copy(cover_hbm, cover, in_sem.at[0]),
            pltpu.make_async_copy(weights_hbm, weights, in_sem.at[1]),
            pltpu.make_async_copy(picks_hbm, picks, in_sem.at[2]),
            pltpu.make_async_copy(cand_hbm.at[pl.ds(0, m // 2)], cands.at[pl.ds(0, m // 2)], in_sem.at[3]),
            pltpu.make_async_copy(points_hbm.at[pl.ds(0, 256)], points.at[pl.ds(0, 256)], in_sem.at[4]),
            pltpu.make_async_copy(points_hbm.at[pl.ds(256, 256)], points.at[pl.ds(256, 256)], in_sem.at[5]),
            pltpu.make_async_copy(points_hbm.at[pl.ds(half, half)], points.at[pl.ds(half, half)], in_sem.at[6]),
            pltpu.make_async_copy(cand_hbm.at[pl.ds(m // 2, m // 2)], cands.at[pl.ds(m // 2, m // 2)], in_sem.at[7]),
        ]
        for copy in copies:
            copy.start()

        others = [k + lax.div(k - me_p + n_pts - 1, n_pts - 1) for k in range(n_pts - 1)]

        near = 4
        beside = [k for k in range(1, n_cand) if min(k, n_cand - k) <= near]
        barrier = pltpu.get_barrier_semaphore()
        for peer in others:
            pl.semaphore_signal(barrier, 1, device_id={"pts": peer}, device_id_type=pl.DeviceIdType.MESH)
        for k in beside:
            pl.semaphore_signal(barrier, 1, device_id={"cand": lax.rem(me_c + k, n_cand)}, device_id_type=pl.DeviceIdType.MESH)

        copies[0].wait()
        copies[1].wait()
        for k in range(8):
            ccol[k * LANES:(k + 1) * LANES, :] = column_of(cover[k:k + 1, :] * 32.0)
            wcol[k * LANES:(k + 1) * LANES, :] = column_of(weights[k:k + 1, :] * (2.0 ** -20))
        copies[2].wait()
        column = (
            me_c * m
            + lax.broadcasted_iota(jnp.int32, (8, LANES), 0) * LANES
            + lax.broadcasted_iota(jnp.int32, (8, LANES), 1)
        )
        mask = jnp.full((8, LANES), -1e30, F32)
        for k in range(TOPK):
            mask = jnp.where(column == picks[k], 0.0, mask)
        bias[...] = mask
        piece = 128
        held = [[results[(2 * q + u) * 4:(2 * q + u) * 4 + 4] for q in range(2)] for u in range(2)]
        for result in results:
            pltpu.matmul_pop(result)
        sums = [jnp.zeros((8, LANES), F32) for _ in range(8)]
        units = [(0, 256, 0, 4), (256, 256, 0, 5), (half, half, 0, 6), (0, half, 2, None), (half, half, 2, None)]
        steps = [(unit, part) for unit in range(len(units)) for part in range(d // 256)]

        def push(step):
            unit, part = steps[step]
            for q in range(2):
                row = (units[unit][2] + q) * 256
                pltpu.matmul_push_rhs(
                    cands[row:row + 256, part * 256:(part + 1) * 256],
                    staging_register=step % 2, mxu_index=q, transpose=True,
                )

        def accumulate(step):
            unit, part = steps[step]
            first, rows, _, _ = units[unit]
            for p in range(rows // piece):
                for q in range(2):
                    pltpu.matmul_acc_lhs(
                        held[unit % 2][q][p],
                        points[first + p * piece:first + (p + 1) * piece, part * 256:(part + 1) * 256],
                        load_staged_rhs=step % 2 if p == 0 else None,
                    )

        def finish(unit):
            first, rows, tile, _ = units[unit]
            for p in range(rows // piece):
                at = slice(first + p * piece, first + (p + 1) * piece)
                high = None
                for q in range(2):
                    sims = pltpu.matmul_pop(held[unit % 2][q][p])
                    for h in range(2):
                        lane = 2 * (tile + q) + h
                        s = sims[:, h * LANES:(h + 1) * LANES]
                        t = jnp.maximum(s - ccol[at, :], 0.0) * wcol[at, :]
                        sums[lane] = sums[lane] + jnp.sum(t.reshape(piece // 8, 8, LANES), axis=0)
                        masked = s + bias[lane:lane + 1, :]
                        high = masked if high is None else jnp.maximum(high, masked)
                maxes[at, :] = jnp.maximum(maxes[at, :], high) if tile else high

        def send_parts(start, size):
            for k in range(start, start + size):
                part_out[k:k + 1, :] = jnp.sum(sums[k], axis=0, keepdims=True)
            part_in[me_p, start:start + size, :] = part_out[start:start + size, :]
            for peer in others:
                pltpu.make_async_remote_copy(
                    part_out.at[pl.ds(start, size)], part_in.at[me_p, pl.ds(start, size)], p_send, p_recv,
                    device_id={"pts": peer}, device_id_type=pl.DeviceIdType.MESH,
                ).start()

        copies[3].wait()
        push(0)
        for step, (unit, part) in enumerate(steps):
            if step + 1 < len(steps):
                if steps[step + 1] == (3, 0):
                    copies[7].wait()
                push(step + 1)
            if part == 0 and units[unit][3] is not None:
                copies[units[unit][3]].wait()
            accumulate(step)
            if part == 2 and unit > 0:
                finish(unit - 1)
        finish(len(units) - 1)
        pl.semaphore_wait(barrier, n_pts - 1 + len(beside))
        send_parts(0, 8)
        reach, rounds = near, 0
        while reach < n_cand // 2:
            for k in (reach, n_cand - reach):
                pl.semaphore_signal(
                    near_sem.at[rounds], 1, device_id={"cand": lax.rem(me_c + k, n_cand)}, device_id_type=pl.DeviceIdType.MESH
                )
            if rounds == 0:
                for k in range(8):
                    high = maxes[k * LANES:(k + 1) * LANES, :].T
                    cov_out[k:k + 1, :] = jnp.max(high, axis=0, keepdims=True) * (2.0 ** -5)
            pl.semaphore_wait(near_sem.at[rounds], 2)
            reach, rounds = 2 * reach, rounds + 1
        for k in along:
            pltpu.make_async_remote_copy(
                cov_out, cov_in.at[k], c_send, c_recv,
                device_id={"cand": lax.rem(me_c + k, n_cand)}, device_id_type=pl.DeviceIdType.MESH,
            ).start()

        some = part_in.at[pl.ds(0, n_pts - 1)]
        pltpu.make_async_copy(some, some, p_recv).wait()
        total = part_in[0]
        for k in range(1, n_pts):
            total = total + part_in[k]
        gains[...] = total
        top_out[...] = best_of_block(gains, col)
        for k in along:
            pltpu.make_async_remote_copy(
                top_out, top_in.at[k], t_send, t_recv.at[int(k == farthest)],
                device_id={"cand": lax.rem(me_c + k, n_cand)}, device_id_type=pl.DeviceIdType.MESH,
            ).start()

        some = cov_in.at[pl.ds(1, n_cand - 1)]
        pltpu.make_async_copy(some, some, c_recv).wait()
        best = jnp.maximum(cover[...], cov_out[...])
        for k in range(1, n_cand):
            best = jnp.maximum(best, cov_in[k])
        for k in range(8):
            gains_refs[k][...] = gains[k:k + 1, :]
            ncov_refs[k][...] = best[k:k + 1, :]

        some = top_in.at[pl.ds(0, n_cand - 2)]
        pltpu.make_async_copy(some, some, t_recv.at[0]).wait()
        top_near[...] = best_of_lists([top_out[...]] + [top_in[k] for k in range(1, n_cand) if k != farthest], col)

        for sent, sem, count in ((part_in, p_send, n_pts - 1), (cov_in, c_send, n_cand - 1), (top_in, t_send, n_cand - 1)):
            some = sent.at[pl.ds(0, count)]
            pltpu.make_async_copy(some, some, sem).wait()

    dma = pltpu.SemaphoreType.DMA
    products = [pltpu.ACC(q)((128, 256), F32) for q in range(2) for _ in range(8)]
    pl.run_scoped(until_last_list, dma((8,)), dma, dma, dma, *products)

    some = top_in.at[pl.ds(farthest, 1)]
    pltpu.make_async_copy(some, some, t_recv.at[1]).wait()
    top_ref[...] = best_of_lists([top_near[...], top_in[farthest]], col)


def write_out(*refs):
    rows, (gains, ncov, top), (gains_all, ncov_all, best, sem) = refs[:17], refs[17:20], refs[20:]
    best[...] = rows[16][:, :TOPK]
    for k in range(8):
        gains_all[k:k + 1, :] = rows[k][...]
        ncov_all[k:k + 1, :] = rows[8 + k][...]
    copies = [
        pltpu.make_async_copy(best, top, sem.at[0]),
        pltpu.make_async_copy(gains_all, gains, sem.at[1]),
        pltpu.make_async_copy(ncov_all, ncov, sem.at[2]),
    ]
    for copy in copies:
        copy.start()
    for copy in copies:
        copy.wait()


def on_device(points, weights, coverage, candidates, picks):
    n_pts, n_cand = lax.axis_size("pts"), lax.axis_size("cand")
    n, d = points.shape
    m = candidates.shape[0]
    hbm = pl.BlockSpec(memory_space=pl.ANY)
    vmem = pl.BlockSpec(memory_space=pltpu.VMEM)
    dma = pltpu.SemaphoreType.DMA
    inside = pl.pallas_call(
        functools.partial(kernel, n_pts, n_cand),
        out_shape=(jax.ShapeDtypeStruct((1, LANES), F32),) * 17,
        in_specs=[hbm] * 5,
        out_specs=(vmem,) * 17,
        scratch_shapes=[
            pltpu.VMEM((n, d), jnp.bfloat16),
            pltpu.VMEM((m, d), jnp.bfloat16),
            pltpu.VMEM((8, LANES), F32),
            pltpu.VMEM((8, LANES), F32),
            pltpu.SMEM((TOPK,), jnp.int32),
            pltpu.VMEM((n, LANES), F32),
            pltpu.VMEM((n, LANES), F32),
            pltpu.VMEM((8, LANES), F32),
            pltpu.VMEM((n, LANES), F32),
            pltpu.VMEM((1024, LANES), F32),
            pltpu.VMEM((8, LANES), F32),
            pltpu.VMEM((n_pts, 8, LANES), F32),
            pltpu.VMEM((8, LANES), F32),
            pltpu.VMEM((n_cand, 8, LANES), F32),
            pltpu.VMEM((1, LANES), F32),
            pltpu.VMEM((n_cand, 1, LANES), F32),
            pltpu.VMEM((1, LANES), F32),
            pltpu.VMEM((8, LANES), F32),
            dma, dma, dma((2,)), pltpu.SemaphoreType.REGULAR((1,)),
        ],
        compiler_params=pltpu.CompilerParams(
            collective_id=0, has_side_effects=True, vmem_limit_bytes=VMEM_BYTES
        ),
        name="facility",
    )(points, weights.reshape(8, LANES), coverage.reshape(8, LANES), candidates, picks)
    gains, ncov, top = pl.pallas_call(
        write_out,
        out_shape=(
            jax.ShapeDtypeStruct((8, LANES), F32),
            jax.ShapeDtypeStruct((8, LANES), F32),
            jax.ShapeDtypeStruct((1, TOPK), F32),
        ),
        in_specs=[vmem] * 17,
        out_specs=(hbm, hbm, hbm),
        scratch_shapes=[
            pltpu.VMEM((8, LANES), F32), pltpu.VMEM((8, LANES), F32), pltpu.VMEM((1, TOPK), F32), dma((3,))
        ],
        compiler_params=pltpu.CompilerParams(vmem_limit_bytes=2**20),
        name="write_out",
    )(*inside)
    return gains.reshape(m), top.reshape(TOPK), ncov.reshape(n)


def solution(mesh):
    placed = (P("pts", None), P("pts"), P("pts"), P("cand", None), P())
    return jax.shard_map(
        on_device, mesh=mesh, in_specs=placed, out_specs=(P("cand"), P(), P("pts")), check_vma=False
    )
```

```python
import functools

import jax
import jax.numpy as jnp
from jax import lax
from jax.experimental import pallas as pl
from jax.experimental.pallas import tpu as pltpu
from jax.sharding import PartitionSpec as P

TOPK = 64
LANES = 128
F32 = jnp.float32
VMEM_BYTES = 56557568 - 70 * 1024


def column_of(row):
    return jnp.broadcast_to(row, (LANES, LANES)).T


def descending(rows):
    rows, n, p = list(rows), len(rows), 1
    while p < n:
        k = p
        while k >= 1:
            for j in range(k % p, n - k, 2 * k):
                for i in range(min(k, n - j - k)):
                    if (i + j) // (2 * p) == (i + j + k) // (2 * p):
                        x, y = rows[i + j], rows[i + j + k]
                        rows[i + j], rows[i + j + k] = jnp.maximum(x, y), jnp.minimum(x, y)
            k //= 2
        p *= 2
    return rows


def wide(row):
    return jnp.broadcast_to(row, (8, LANES))


def added(terms):
    while len(terms) > 1:
        terms = [x + y for x, y in zip(terms[::2], terms[1::2])] + ([terms[-1]] if len(terms) % 2 else [])
    return terms[0]


def number_above(columns, row):
    total = added([jnp.where(column > row, 1.0, 0.0) for column in columns])
    return wide(jnp.sum(total, axis=0, keepdims=True))


def placed(pairs, blocks, sub):
    result = []
    for block in range(blocks):
        place = sub + float(block * 8)
        best = jnp.full((8, LANES), jnp.inf, F32)
        for row, above in pairs:
            best = jnp.minimum(best, jnp.where(above <= place, row, jnp.inf))
        result.append(jnp.broadcast_to(jnp.min(best, axis=1, keepdims=True), (8, LANES)))
    return result


def as_row(blocks, sub, lane):
    total = added([jnp.where(lane == sub + float(index * 8), block, 0.0) for index, block in enumerate(blocks)])
    return jnp.sum(total, axis=0, keepdims=True)


def positions():
    sub = lax.broadcasted_iota(jnp.int32, (8, LANES), 0).astype(F32)
    lane = lax.broadcasted_iota(jnp.int32, (8, LANES), 1)
    return sub, lane.astype(F32), lax.rem(lane, TOPK).astype(F32)


def order_pair(rows, columns):
    sub, _, twice = positions()
    pairs = [(wide(row), number_above(columns, wide(row))) for row in rows]
    return as_row(placed(pairs, TOPK // 8, sub), sub, twice)


def best_of_block(total_ref, col_ref):
    sub, lane, _ = positions()
    rows = descending([total_ref[k:k + 1, :] for k in range(8)])
    ranked = ((0, (0,)), (1, (1, 2)), (3, (3, 4, 5, 6, 7)))
    for k, _ in ranked:
        col_ref[k * LANES:(k + 1) * LANES, :] = column_of(rows[k])
    kept = []
    for k, taken in ranked:
        row = wide(rows[k])
        columns = [col_ref[k * LANES + 8 * j:k * LANES + 8 * j + 8, :] for j in range(16)]
        blocks = TOPK // (k + 1) // 8
        if taken == (k,):
            kept += placed([(row, number_above(columns, row))], blocks, sub)
            continue
        before = [
            jnp.where((column > row) | ((column == row) & (sub + float(8 * j) < lane)), 1.0, 0.0)
            for j, column in enumerate(columns)
        ]
        rank = wide(jnp.sum(added(before), axis=0, keepdims=True))
        for block in range(blocks):
            here = rank == sub + float(8 * block)
            for r in taken:
                best = jnp.max(jnp.where(here, wide(rows[r]), -jnp.inf), axis=1, keepdims=True)
                kept.append(jnp.broadcast_to(best, (8, LANES)))
    first = as_row(kept[:16], sub, lane)
    second = jnp.where(lane[:1] < 8.0 * (len(kept) - 16), as_row(kept[16:], sub, lane), -jnp.inf)
    return order_pair([first, second], kept)


def best_of_lists(lists, col_ref):
    lane = lax.broadcasted_iota(jnp.int32, (1, LANES), 1)
    rows = descending(lists)
    low = jnp.full((1, LANES), -jnp.inf, F32)
    packed = []
    for group in ((0, 1, 2, 5), (3, 4) + tuple(range(6, len(rows)))):
        at, line = 0, low
        for s in group:
            if s < len(rows):
                count = TOPK // (s + 1)
                moved = rows[s] if at % TOPK == 0 else pltpu.roll(rows[s], at, 1)
                line = jnp.where((lane >= at) & (lane < at + count), moved, line)
                at += count
        if at:
            packed.append((line, at))
    columns = []
    for k, (line, used) in enumerate(packed):
        col_ref[k * LANES:(k + 1) * LANES, :] = column_of(line)
        columns += [col_ref[k * LANES + 8 * j:k * LANES + 8 * j + 8, :] for j in range(-(-used // 8))]
    return order_pair([line for line, _ in packed], columns)


def kernel(n_pts, n_cand, points_hbm, weights_hbm, cover_hbm, cand_hbm, picks_hbm, *refs):
    gains_refs, ncov_refs, top_ref = refs[:8], refs[8:16], refs[16]
    (
        points, cands, weights, cover, picks, wcol, ccol, bias, maxes, col,
        part_out, part_in, cov_out, cov_in, top_out, top_in, top_near, gains,
        p_recv, c_recv, t_recv, near_sem,
    ) = refs[17:]
    farthest = n_cand // 2

    def until_last_list(in_sem, p_send, c_send, t_send, *results):
        n, d = points.shape
        m = cands.shape[0]
        me_p = lax.axis_index("pts")
        me_c = lax.axis_index("cand")

        half = n // 2
        along = sorted(range(1, n_cand), key=lambda k: -min(k, n_cand - k))
        copies = [
            pltpu.make_async_copy(cover_hbm, cover, in_sem.at[0]),
            pltpu.make_async_copy(weights_hbm, weights, in_sem.at[1]),
            pltpu.make_async_copy(picks_hbm, picks, in_sem.at[2]),
            pltpu.make_async_copy(cand_hbm.at[pl.ds(0, m // 2)], cands.at[pl.ds(0, m // 2)], in_sem.at[3]),
            pltpu.make_async_copy(points_hbm.at[pl.ds(0, 256)], points.at[pl.ds(0, 256)], in_sem.at[4]),
            pltpu.make_async_copy(points_hbm.at[pl.ds(256, 256)], points.at[pl.ds(256, 256)], in_sem.at[5]),
            pltpu.make_async_copy(points_hbm.at[pl.ds(half, half)], points.at[pl.ds(half, half)], in_sem.at[6]),
            pltpu.make_async_copy(cand_hbm.at[pl.ds(m // 2, m // 2)], cands.at[pl.ds(m // 2, m // 2)], in_sem.at[7]),
        ]
        for copy in copies:
            copy.start()

        others = [k + lax.div(k - me_p + n_pts - 1, n_pts - 1) for k in range(n_pts - 1)]

        near = 4
        beside = [k for k in range(1, n_cand) if min(k, n_cand - k) <= near]
        barrier = pltpu.get_barrier_semaphore()
        for peer in others:
            pl.semaphore_signal(barrier, 1, device_id={"pts": peer}, device_id_type=pl.DeviceIdType.MESH)
        for k in beside:
            pl.semaphore_signal(barrier, 1, device_id={"cand": lax.rem(me_c + k, n_cand)}, device_id_type=pl.DeviceIdType.MESH)

        copies[0].wait()
        copies[1].wait()
        for k in range(8):
            ccol[k * LANES:(k + 1) * LANES, :] = column_of(cover[k:k + 1, :] * 32.0)
            wcol[k * LANES:(k + 1) * LANES, :] = column_of(weights[k:k + 1, :] * (2.0 ** -20))
        copies[2].wait()
        column = (
            me_c * m
            + lax.broadcasted_iota(jnp.int32, (8, LANES), 0) * LANES
            + lax.broadcasted_iota(jnp.int32, (8, LANES), 1)
        )
        mask = jnp.full((8, LANES), -1e30, F32)
        for k in range(TOPK):
            mask = jnp.where(column == picks[k], 0.0, mask)
        bias[...] = mask
        piece = 128
        held = [[results[(2 * q + u) * 4:(2 * q + u) * 4 + 4] for q in range(2)] for u in range(2)]
        for result in results:
            pltpu.matmul_pop(result)
        sums = [jnp.zeros((8, LANES), F32) for _ in range(8)]
        units = [(0, 256, 0, 4), (256, 256, 0, 5), (half, half, 0, 6), (0, half, 2, None), (half, half, 2, None)]
        steps = [(unit, part) for unit in range(len(units)) for part in range(d // 256)]

        def push(step):
            unit, part = steps[step]
            for q in range(2):
                row = (units[unit][2] + q) * 256
                pltpu.matmul_push_rhs(
                    cands[row:row + 256, part * 256:(part + 1) * 256],
                    staging_register=step % 2, mxu_index=q, transpose=True,
                )

        def accumulate(step):
            unit, part = steps[step]
            first, rows, _, _ = units[unit]
            for p in range(rows // piece):
                for q in range(2):
                    pltpu.matmul_acc_lhs(
                        held[unit % 2][q][p],
                        points[first + p * piece:first + (p + 1) * piece, part * 256:(part + 1) * 256],
                        load_staged_rhs=step % 2 if p == 0 else None,
                    )

        def finish(unit):
            first, rows, tile, _ = units[unit]
            for p in range(rows // piece):
                at = slice(first + p * piece, first + (p + 1) * piece)
                high = None
                for q in range(2):
                    sims = pltpu.matmul_pop(held[unit % 2][q][p])
                    for h in range(2):
                        lane = 2 * (tile + q) + h
                        s = sims[:, h * LANES:(h + 1) * LANES]
                        t = jnp.maximum(s - ccol[at, :], 0.0) * wcol[at, :]
                        sums[lane] = sums[lane] + jnp.sum(t.reshape(piece // 8, 8, LANES), axis=0)
                        masked = s + bias[lane:lane + 1, :]
                        high = masked if high is None else jnp.maximum(high, masked)
                maxes[at, :] = jnp.maximum(maxes[at, :], high) if tile else high

        def send_parts(start, size):
            for k in range(start, start + size):
                part_out[k:k + 1, :] = jnp.sum(sums[k], axis=0, keepdims=True)
            part_in[me_p, start:start + size, :] = part_out[start:start + size, :]
            for peer in others:
                pltpu.make_async_remote_copy(
                    part_out.at[pl.ds(start, size)], part_in.at[me_p, pl.ds(start, size)], p_send, p_recv,
                    device_id={"pts": peer}, device_id_type=pl.DeviceIdType.MESH,
                ).start()

        copies[3].wait()
        push(0)
        for step, (unit, part) in enumerate(steps):
            if step + 1 < len(steps):
                if steps[step + 1] == (3, 0):
                    copies[7].wait()
                push(step + 1)
            if part == 0 and units[unit][3] is not None:
                copies[units[unit][3]].wait()
            accumulate(step)
            if part == 2 and unit > 0:
                finish(unit - 1)
        finish(len(units) - 1)
        pl.semaphore_wait(barrier, n_pts - 1 + len(beside))
        send_parts(0, 8)
        reach, rounds = near, 0
        while reach < n_cand // 2:
            for k in (reach, n_cand - reach):
                pl.semaphore_signal(
                    near_sem.at[rounds], 1, device_id={"cand": lax.rem(me_c + k, n_cand)}, device_id_type=pl.DeviceIdType.MESH
                )
            if rounds == 0:
                for k in range(8):
                    high = maxes[k * LANES:(k + 1) * LANES, :].T
                    cov_out[k:k + 1, :] = jnp.max(high, axis=0, keepdims=True) * (2.0 ** -5)
            pl.semaphore_wait(near_sem.at[rounds], 2)
            reach, rounds = 2 * reach, rounds + 1
        for k in along:
            pltpu.make_async_remote_copy(
                cov_out, cov_in.at[k], c_send, c_recv,
                device_id={"cand": lax.rem(me_c + k, n_cand)}, device_id_type=pl.DeviceIdType.MESH,
            ).start()

        some = part_in.at[pl.ds(0, n_pts - 1)]
        pltpu.make_async_copy(some, some, p_recv).wait()
        total = added([part_in[k] for k in range(n_pts)])
        gains[...] = total
        top_out[...] = best_of_block(gains, col)
        for k in along:
            pltpu.make_async_remote_copy(
                top_out, top_in.at[k], t_send, t_recv.at[int(k == farthest)],
                device_id={"cand": lax.rem(me_c + k, n_cand)}, device_id_type=pl.DeviceIdType.MESH,
            ).start()

        some = cov_in.at[pl.ds(1, n_cand - 1)]
        pltpu.make_async_copy(some, some, c_recv).wait()
        best = jnp.maximum(cover[...], cov_out[...])
        for k in range(1, n_cand):
            best = jnp.maximum(best, cov_in[k])
        for k in range(8):
            gains_refs[k][...] = gains[k:k + 1, :]
            ncov_refs[k][...] = best[k:k + 1, :]

        some = top_in.at[pl.ds(0, n_cand - 2)]
        pltpu.make_async_copy(some, some, t_recv.at[0]).wait()
        top_near[...] = best_of_lists([top_out[...]] + [top_in[k] for k in range(1, n_cand) if k != farthest], col)

        for sent, sem, count in ((part_in, p_send, n_pts - 1), (cov_in, c_send, n_cand - 1), (top_in, t_send, n_cand - 1)):
            some = sent.at[pl.ds(0, count)]
            pltpu.make_async_copy(some, some, sem).wait()

    dma = pltpu.SemaphoreType.DMA
    products = [pltpu.ACC(q)((128, 256), F32) for q in range(2) for _ in range(8)]
    pl.run_scoped(until_last_list, dma((8,)), dma, dma, dma, *products)

    some = top_in.at[pl.ds(farthest, 1)]
    pltpu.make_async_copy(some, some, t_recv.at[1]).wait()
    top_ref[...] = best_of_lists([top_near[...], top_in[farthest]], col)


def write_out(*refs):
    rows, (gains, ncov, top), (gains_all, ncov_all, best) = refs[:17], refs[17:20], refs[20:]
    best[...] = rows[16][:, :TOPK]
    for k in range(8):
        gains_all[k:k + 1, :] = rows[k][...]
        ncov_all[k:k + 1, :] = rows[8 + k][...]

    def send(sem):
        copies = [
            pltpu.make_async_copy(best, top, sem.at[0]),
            pltpu.make_async_copy(gains_all, gains, sem.at[1]),
            pltpu.make_async_copy(ncov_all, ncov, sem.at[2]),
        ]
        for copy in copies:
            copy.start()
        for copy in copies:
            copy.wait()

    pl.run_scoped(send, pltpu.SemaphoreType.DMA((3,)))


def on_device(points, weights, coverage, candidates, picks):
    n_pts, n_cand = lax.axis_size("pts"), lax.axis_size("cand")
    n, d = points.shape
    m = candidates.shape[0]
    hbm = pl.BlockSpec(memory_space=pl.ANY)
    vmem = pl.BlockSpec(memory_space=pltpu.VMEM)
    dma = pltpu.SemaphoreType.DMA
    inside = pl.pallas_call(
        functools.partial(kernel, n_pts, n_cand),
        out_shape=(jax.ShapeDtypeStruct((1, LANES), F32),) * 17,
        in_specs=[hbm] * 5,
        out_specs=(vmem,) * 17,
        scratch_shapes=[
            pltpu.VMEM((n, d), jnp.bfloat16),
            pltpu.VMEM((m, d), jnp.bfloat16),
            pltpu.VMEM((8, LANES), F32),
            pltpu.VMEM((8, LANES), F32),
            pltpu.SMEM((TOPK,), jnp.int32),
            pltpu.VMEM((n, LANES), F32),
            pltpu.VMEM((n, LANES), F32),
            pltpu.VMEM((8, LANES), F32),
            pltpu.VMEM((n, LANES), F32),
            pltpu.VMEM((1024, LANES), F32),
            pltpu.VMEM((8, LANES), F32),
            pltpu.VMEM((n_pts, 8, LANES), F32),
            pltpu.VMEM((8, LANES), F32),
            pltpu.VMEM((n_cand, 8, LANES), F32),
            pltpu.VMEM((1, LANES), F32),
            pltpu.VMEM((n_cand, 1, LANES), F32),
            pltpu.VMEM((1, LANES), F32),
            pltpu.VMEM((8, LANES), F32),
            dma, dma, dma((2,)), pltpu.SemaphoreType.REGULAR((1,)),
        ],
        compiler_params=pltpu.CompilerParams(
            collective_id=0, has_side_effects=True, vmem_limit_bytes=VMEM_BYTES
        ),
        name="facility",
    )(points, weights.reshape(8, LANES), coverage.reshape(8, LANES), candidates, picks)
    gains, ncov, top = pl.pallas_call(
        write_out,
        out_shape=(
            jax.ShapeDtypeStruct((8, LANES), F32),
            jax.ShapeDtypeStruct((8, LANES), F32),
            jax.ShapeDtypeStruct((1, TOPK), F32),
        ),
        in_specs=[vmem] * 17,
        out_specs=(hbm, hbm, hbm),
        scratch_shapes=[
            pltpu.VMEM((8, LANES), F32), pltpu.VMEM((8, LANES), F32), pltpu.VMEM((1, TOPK), F32)
        ],
        compiler_params=pltpu.CompilerParams(vmem_limit_bytes=2**20),
        name="write_out",
    )(*inside)
    return gains.reshape(m), top.reshape(TOPK), ncov.reshape(n)


def solution(mesh):
    placed = (P("pts", None), P("pts"), P("pts"), P("cand", None), P())
    return jax.shard_map(
        on_device, mesh=mesh, in_specs=placed, out_specs=(P("cand"), P(), P("pts")), check_vma=False
    )
```

```python
import functools

import jax
import jax.numpy as jnp
from jax import lax
from jax.experimental import pallas as pl
from jax.experimental.pallas import tpu as pltpu
from jax.sharding import PartitionSpec as P

TOPK = 64
LANES = 128
F32 = jnp.float32
VMEM_BYTES = 56557568 - 70 * 1024


def column_of(row):
    return jnp.broadcast_to(row, (LANES, LANES)).T


def descending(rows):
    rows, n, p = list(rows), len(rows), 1
    while p < n:
        k = p
        while k >= 1:
            for j in range(k % p, n - k, 2 * k):
                for i in range(min(k, n - j - k)):
                    if (i + j) // (2 * p) == (i + j + k) // (2 * p):
                        x, y = rows[i + j], rows[i + j + k]
                        rows[i + j], rows[i + j + k] = jnp.maximum(x, y), jnp.minimum(x, y)
            k //= 2
        p *= 2
    return rows


def wide(row):
    return jnp.broadcast_to(row, (8, LANES))


def added(terms):
    while len(terms) > 1:
        terms = [x + y for x, y in zip(terms[::2], terms[1::2])] + ([terms[-1]] if len(terms) % 2 else [])
    return terms[0]


def number_above(columns, row):
    total = added([jnp.where(column > row, 1.0, 0.0) for column in columns])
    return wide(jnp.sum(total, axis=0, keepdims=True))


def placed(pairs, blocks, sub):
    result = []
    for block in range(blocks):
        place = sub + float(block * 8)
        best = jnp.full((8, LANES), jnp.inf, F32)
        for row, above in pairs:
            best = jnp.minimum(best, jnp.where(above <= place, row, jnp.inf))
        result.append(jnp.broadcast_to(jnp.min(best, axis=1, keepdims=True), (8, LANES)))
    return result


def as_row(blocks, sub, lane):
    total = added([jnp.where(lane == sub + float(index * 8), block, 0.0) for index, block in enumerate(blocks)])
    return jnp.sum(total, axis=0, keepdims=True)


def positions():
    sub = lax.broadcasted_iota(jnp.int32, (8, LANES), 0).astype(F32)
    lane = lax.broadcasted_iota(jnp.int32, (8, LANES), 1)
    return sub, lane.astype(F32), lax.rem(lane, TOPK).astype(F32)


def order_pair(rows, columns):
    sub, _, twice = positions()
    pairs = [(wide(row), number_above(columns, wide(row))) for row in rows]
    return as_row(placed(pairs, TOPK // 8, sub), sub, twice)


def best_of_block(total_ref, col_ref):
    sub, lane, _ = positions()
    rows = descending([total_ref[k:k + 1, :] for k in range(8)])
    ranked = ((0, (0,)), (1, (1, 2)), (3, (3, 4, 5, 6, 7)))
    for k, _ in ranked:
        col_ref[k * LANES:(k + 1) * LANES, :] = column_of(rows[k])
    kept = []
    for k, taken in ranked:
        row = wide(rows[k])
        columns = [col_ref[k * LANES + 8 * j:k * LANES + 8 * j + 8, :] for j in range(16)]
        blocks = TOPK // (k + 1) // 8
        if taken == (k,):
            kept += placed([(row, number_above(columns, row))], blocks, sub)
            continue
        before = [
            jnp.where((column > row) | ((column == row) & (sub + float(8 * j) < lane)), 1.0, 0.0)
            for j, column in enumerate(columns)
        ]
        rank = wide(jnp.sum(added(before), axis=0, keepdims=True))
        for block in range(blocks):
            here = rank == sub + float(8 * block)
            for r in taken:
                best = jnp.max(jnp.where(here, wide(rows[r]), -jnp.inf), axis=1, keepdims=True)
                kept.append(jnp.broadcast_to(best, (8, LANES)))
    first = as_row(kept[:16], sub, lane)
    second = jnp.where(lane[:1] < 8.0 * (len(kept) - 16), as_row(kept[16:], sub, lane), -jnp.inf)
    return order_pair([first, second], kept)


def best_of_lists(lists, col_ref):
    lane = lax.broadcasted_iota(jnp.int32, (1, LANES), 1)
    rows = descending(lists)
    low = jnp.full((1, LANES), -jnp.inf, F32)
    packed = []
    for group in ((0, 1, 2, 5), (3, 4) + tuple(range(6, len(rows)))):
        at, line = 0, low
        for s in group:
            if s < len(rows):
                count = TOPK // (s + 1)
                moved = rows[s] if at % TOPK == 0 else pltpu.roll(rows[s], at, 1)
                line = jnp.where((lane >= at) & (lane < at + count), moved, line)
                at += count
        if at:
            packed.append((line, at))
    columns = []
    for k, (line, used) in enumerate(packed):
        col_ref[k * LANES:(k + 1) * LANES, :] = column_of(line)
        columns += [col_ref[k * LANES + 8 * j:k * LANES + 8 * j + 8, :] for j in range(-(-used // 8))]
    return order_pair([line for line, _ in packed], columns)


def merge_last(far, near_columns):
    sub, lane, twice = positions()
    row, first = wide(far), lane < float(TOPK)
    parts, ahead = [], []
    for block, column in enumerate(near_columns):
        count = jnp.sum(jnp.where((row > column) & first, 1.0, 0.0), axis=1, keepdims=True)
        parts.append(jnp.where(count + sub + float(8 * block) == lane, column, 0.0))
        ahead.append(jnp.where(column >= row, 1.0, 0.0))
    place = wide(jnp.sum(added(ahead), axis=0, keepdims=True)) + twice
    for block in range(TOPK // 8):
        slot = sub + float(8 * block)
        value = jnp.sum(jnp.where((place == slot) & first, row, 0.0), axis=1, keepdims=True)
        parts.append(jnp.where(lane == slot, value, 0.0))
    return jnp.sum(added(parts), axis=0, keepdims=True)


def kernel(n_pts, n_cand, points_hbm, weights_hbm, cover_hbm, cand_hbm, picks_hbm, *refs):
    gains_refs, ncov_refs, top_ref = refs[:8], refs[8:16], refs[16]
    (
        points, cands, weights, cover, picks, wcol, ccol, bias, maxes, col,
        part_out, part_in, cov_out, cov_in, top_out, top_in, near_columns, gains,
        p_recv, c_recv, t_recv, near_sem,
    ) = refs[17:]
    farthest = n_cand // 2

    def until_last_list(in_sem, p_send, c_send, t_send, *results):
        n, d = points.shape
        m = cands.shape[0]
        me_p = lax.axis_index("pts")
        me_c = lax.axis_index("cand")

        half = n // 2
        along = sorted(range(1, n_cand), key=lambda k: -min(k, n_cand - k))
        copies = [
            pltpu.make_async_copy(cover_hbm, cover, in_sem.at[0]),
            pltpu.make_async_copy(weights_hbm, weights, in_sem.at[1]),
            pltpu.make_async_copy(picks_hbm, picks, in_sem.at[2]),
            pltpu.make_async_copy(cand_hbm.at[pl.ds(0, m // 2)], cands.at[pl.ds(0, m // 2)], in_sem.at[3]),
            pltpu.make_async_copy(points_hbm.at[pl.ds(0, 256)], points.at[pl.ds(0, 256)], in_sem.at[4]),
            pltpu.make_async_copy(points_hbm.at[pl.ds(256, 256)], points.at[pl.ds(256, 256)], in_sem.at[5]),
            pltpu.make_async_copy(points_hbm.at[pl.ds(half, half)], points.at[pl.ds(half, half)], in_sem.at[6]),
            pltpu.make_async_copy(cand_hbm.at[pl.ds(m // 2, m // 2)], cands.at[pl.ds(m // 2, m // 2)], in_sem.at[7]),
        ]
        for copy in copies:
            copy.start()

        others = [k + lax.div(k - me_p + n_pts - 1, n_pts - 1) for k in range(n_pts - 1)]

        near = 4
        beside = [k for k in range(1, n_cand) if min(k, n_cand - k) <= near]
        barrier = pltpu.get_barrier_semaphore()
        for peer in others:
            pl.semaphore_signal(barrier, 1, device_id={"pts": peer}, device_id_type=pl.DeviceIdType.MESH)
        for k in beside:
            pl.semaphore_signal(barrier, 1, device_id={"cand": lax.rem(me_c + k, n_cand)}, device_id_type=pl.DeviceIdType.MESH)

        copies[0].wait()
        copies[1].wait()
        for k in range(8):
            ccol[k * LANES:(k + 1) * LANES, :] = column_of(cover[k:k + 1, :] * 32.0)
            wcol[k * LANES:(k + 1) * LANES, :] = column_of(weights[k:k + 1, :] * (2.0 ** -20))
        copies[2].wait()
        column = (
            me_c * m
            + lax.broadcasted_iota(jnp.int32, (8, LANES), 0) * LANES
            + lax.broadcasted_iota(jnp.int32, (8, LANES), 1)
        )
        mask = jnp.full((8, LANES), -1e30, F32)
        for k in range(TOPK):
            mask = jnp.where(column == picks[k], 0.0, mask)
        bias[...] = mask
        piece = 128
        held = [[results[(2 * q + u) * 4:(2 * q + u) * 4 + 4] for q in range(2)] for u in range(2)]
        for result in results:
            pltpu.matmul_pop(result)
        sums = [jnp.zeros((8, LANES), F32) for _ in range(8)]
        units = [(0, 256, 0, 4), (256, 256, 0, 5), (half, half, 0, 6), (0, half, 2, None), (half, half, 2, None)]
        steps = [(unit, part) for unit in range(len(units)) for part in range(d // 256)]

        def push(step):
            unit, part = steps[step]
            for q in range(2):
                row = (units[unit][2] + q) * 256
                pltpu.matmul_push_rhs(
                    cands[row:row + 256, part * 256:(part + 1) * 256],
                    staging_register=step % 2, mxu_index=q, transpose=True,
                )

        def accumulate(step):
            unit, part = steps[step]
            first, rows, _, _ = units[unit]
            for p in range(rows // piece):
                for q in range(2):
                    pltpu.matmul_acc_lhs(
                        held[unit % 2][q][p],
                        points[first + p * piece:first + (p + 1) * piece, part * 256:(part + 1) * 256],
                        load_staged_rhs=step % 2 if p == 0 else None,
                    )

        def finish(unit):
            first, rows, tile, _ = units[unit]
            for p in range(rows // piece):
                at = slice(first + p * piece, first + (p + 1) * piece)
                high = None
                for q in range(2):
                    sims = pltpu.matmul_pop(held[unit % 2][q][p])
                    for h in range(2):
                        lane = 2 * (tile + q) + h
                        s = sims[:, h * LANES:(h + 1) * LANES]
                        t = jnp.maximum(s - ccol[at, :], 0.0) * wcol[at, :]
                        sums[lane] = sums[lane] + jnp.sum(t.reshape(piece // 8, 8, LANES), axis=0)
                        masked = s + bias[lane:lane + 1, :]
                        high = masked if high is None else jnp.maximum(high, masked)
                maxes[at, :] = jnp.maximum(maxes[at, :], high) if tile else high

        def send_parts(start, size):
            for k in range(start, start + size):
                part_out[k:k + 1, :] = jnp.sum(sums[k], axis=0, keepdims=True)
            part_in[me_p, start:start + size, :] = part_out[start:start + size, :]
            for peer in others:
                pltpu.make_async_remote_copy(
                    part_out.at[pl.ds(start, size)], part_in.at[me_p, pl.ds(start, size)], p_send, p_recv,
                    device_id={"pts": peer}, device_id_type=pl.DeviceIdType.MESH,
                ).start()

        copies[3].wait()
        push(0)
        for step, (unit, part) in enumerate(steps):
            if step + 1 < len(steps):
                if steps[step + 1] == (3, 0):
                    copies[7].wait()
                push(step + 1)
            if part == 0 and units[unit][3] is not None:
                copies[units[unit][3]].wait()
            accumulate(step)
            if part == 2 and unit > 0:
                finish(unit - 1)
        finish(len(units) - 1)
        pl.semaphore_wait(barrier, n_pts - 1 + len(beside))
        send_parts(0, 8)
        reach, rounds = near, 0
        while reach < n_cand // 2:
            for k in (reach, n_cand - reach):
                pl.semaphore_signal(
                    near_sem.at[rounds], 1, device_id={"cand": lax.rem(me_c + k, n_cand)}, device_id_type=pl.DeviceIdType.MESH
                )
            if rounds == 0:
                for k in range(8):
                    high = maxes[k * LANES:(k + 1) * LANES, :].T
                    cov_out[k:k + 1, :] = jnp.max(high, axis=0, keepdims=True) * (2.0 ** -5)
            pl.semaphore_wait(near_sem.at[rounds], 2)
            reach, rounds = 2 * reach, rounds + 1
        for k in along:
            pltpu.make_async_remote_copy(
                cov_out, cov_in.at[k], c_send, c_recv,
                device_id={"cand": lax.rem(me_c + k, n_cand)}, device_id_type=pl.DeviceIdType.MESH,
            ).start()

        some = part_in.at[pl.ds(0, n_pts - 1)]
        pltpu.make_async_copy(some, some, p_recv).wait()
        total = added([part_in[k] for k in range(n_pts)])
        gains[...] = total
        top_out[...] = best_of_block(gains, col)
        for k in along:
            pltpu.make_async_remote_copy(
                top_out, top_in.at[k], t_send, t_recv.at[int(k == farthest)],
                device_id={"cand": lax.rem(me_c + k, n_cand)}, device_id_type=pl.DeviceIdType.MESH,
            ).start()

        some = cov_in.at[pl.ds(1, n_cand - 1)]
        pltpu.make_async_copy(some, some, c_recv).wait()
        best = jnp.maximum(cover[...], cov_out[...])
        for k in range(1, n_cand):
            best = jnp.maximum(best, cov_in[k])
        for k in range(8):
            gains_refs[k][...] = gains[k:k + 1, :]
            ncov_refs[k][...] = best[k:k + 1, :]

        some = top_in.at[pl.ds(0, n_cand - 2)]
        pltpu.make_async_copy(some, some, t_recv.at[0]).wait()
        near = best_of_lists([top_out[...]] + [top_in[k] for k in range(1, n_cand) if k != farthest], col)
        near_columns[...] = column_of(near)[:TOPK, :]

        for sent, sem, count in ((part_in, p_send, n_pts - 1), (cov_in, c_send, n_cand - 1), (top_in, t_send, n_cand - 1)):
            some = sent.at[pl.ds(0, count)]
            pltpu.make_async_copy(some, some, sem).wait()

    dma = pltpu.SemaphoreType.DMA
    products = [pltpu.ACC(q)((128, 256), F32) for q in range(2) for _ in range(8)]
    pl.run_scoped(until_last_list, dma((8,)), dma, dma, dma, *products)

    some = top_in.at[pl.ds(farthest, 1)]
    pltpu.make_async_copy(some, some, t_recv.at[1]).wait()
    top_ref[...] = merge_last(top_in[farthest], [near_columns[k:k + 8, :] for k in range(0, TOPK, 8)])


def write_out(*refs):
    rows, (gains, ncov, top), (gains_all, ncov_all, best) = refs[:17], refs[17:20], refs[20:]
    best[...] = rows[16][:, :TOPK]
    for k in range(8):
        gains_all[k:k + 1, :] = rows[k][...]
        ncov_all[k:k + 1, :] = rows[8 + k][...]

    def send(sem):
        copies = [
            pltpu.make_async_copy(best, top, sem.at[0]),
            pltpu.make_async_copy(gains_all, gains, sem.at[1]),
            pltpu.make_async_copy(ncov_all, ncov, sem.at[2]),
        ]
        for copy in copies:
            copy.start()
        for copy in copies:
            copy.wait()

    pl.run_scoped(send, pltpu.SemaphoreType.DMA((3,)))


def on_device(points, weights, coverage, candidates, picks):
    n_pts, n_cand = lax.axis_size("pts"), lax.axis_size("cand")
    n, d = points.shape
    m = candidates.shape[0]
    hbm = pl.BlockSpec(memory_space=pl.ANY)
    vmem = pl.BlockSpec(memory_space=pltpu.VMEM)
    dma = pltpu.SemaphoreType.DMA
    inside = pl.pallas_call(
        functools.partial(kernel, n_pts, n_cand),
        out_shape=(jax.ShapeDtypeStruct((1, LANES), F32),) * 17,
        in_specs=[hbm] * 5,
        out_specs=(vmem,) * 17,
        scratch_shapes=[
            pltpu.VMEM((n, d), jnp.bfloat16),
            pltpu.VMEM((m, d), jnp.bfloat16),
            pltpu.VMEM((8, LANES), F32),
            pltpu.VMEM((8, LANES), F32),
            pltpu.SMEM((TOPK,), jnp.int32),
            pltpu.VMEM((n, LANES), F32),
            pltpu.VMEM((n, LANES), F32),
            pltpu.VMEM((8, LANES), F32),
            pltpu.VMEM((n, LANES), F32),
            pltpu.VMEM((1024, LANES), F32),
            pltpu.VMEM((8, LANES), F32),
            pltpu.VMEM((n_pts, 8, LANES), F32),
            pltpu.VMEM((8, LANES), F32),
            pltpu.VMEM((n_cand, 8, LANES), F32),
            pltpu.VMEM((1, LANES), F32),
            pltpu.VMEM((n_cand, 1, LANES), F32),
            pltpu.VMEM((TOPK, LANES), F32),
            pltpu.VMEM((8, LANES), F32),
            dma, dma, dma((2,)), pltpu.SemaphoreType.REGULAR((1,)),
        ],
        compiler_params=pltpu.CompilerParams(
            collective_id=0, has_side_effects=True, vmem_limit_bytes=VMEM_BYTES
        ),
        name="facility",
    )(points, weights.reshape(8, LANES), coverage.reshape(8, LANES), candidates, picks)
    gains, ncov, top = pl.pallas_call(
        write_out,
        out_shape=(
            jax.ShapeDtypeStruct((8, LANES), F32),
            jax.ShapeDtypeStruct((8, LANES), F32),
            jax.ShapeDtypeStruct((1, TOPK), F32),
        ),
        in_specs=[vmem] * 17,
        out_specs=(hbm, hbm, hbm),
        scratch_shapes=[
            pltpu.VMEM((8, LANES), F32), pltpu.VMEM((8, LANES), F32), pltpu.VMEM((1, TOPK), F32)
        ],
        compiler_params=pltpu.CompilerParams(vmem_limit_bytes=2**20),
        name="write_out",
    )(*inside)
    return gains.reshape(m), top.reshape(TOPK), ncov.reshape(n)


def solution(mesh):
    placed = (P("pts", None), P("pts"), P("pts"), P("cand", None), P())
    return jax.shard_map(
        on_device, mesh=mesh, in_specs=placed, out_specs=(P("cand"), P(), P("pts")), check_vma=False
    )
```

```python
import functools

import jax
import jax.numpy as jnp
from jax import lax
from jax.experimental import pallas as pl
from jax.experimental.pallas import tpu as pltpu
from jax.sharding import PartitionSpec as P

TOPK = 64
LANES = 128
F32 = jnp.float32
VMEM_BYTES = 56557568 - 70 * 1024


def column_of(row):
    return jnp.broadcast_to(row, (LANES, LANES)).T


def descending(rows):
    rows, n, p = list(rows), len(rows), 1
    while p < n:
        k = p
        while k >= 1:
            for j in range(k % p, n - k, 2 * k):
                for i in range(min(k, n - j - k)):
                    if (i + j) // (2 * p) == (i + j + k) // (2 * p):
                        x, y = rows[i + j], rows[i + j + k]
                        rows[i + j], rows[i + j + k] = jnp.maximum(x, y), jnp.minimum(x, y)
            k //= 2
        p *= 2
    return rows


def wide(row):
    return jnp.broadcast_to(row, (8, LANES))


def added(terms):
    while len(terms) > 1:
        terms = [x + y for x, y in zip(terms[::2], terms[1::2])] + ([terms[-1]] if len(terms) % 2 else [])
    return terms[0]


def number_above(columns, row):
    total = added([jnp.where(column > row, 1.0, 0.0) for column in columns])
    return wide(jnp.sum(total, axis=0, keepdims=True))


def placed(pairs, blocks, sub):
    result = []
    for block in range(blocks):
        place = sub + float(block * 8)
        best = jnp.full((8, LANES), jnp.inf, F32)
        for row, above in pairs:
            best = jnp.minimum(best, jnp.where(above <= place, row, jnp.inf))
        result.append(jnp.broadcast_to(jnp.min(best, axis=1, keepdims=True), (8, LANES)))
    return result


def as_row(blocks, sub, lane):
    total = added([jnp.where(lane == sub + float(index * 8), block, 0.0) for index, block in enumerate(blocks)])
    return jnp.sum(total, axis=0, keepdims=True)


def positions():
    sub = lax.broadcasted_iota(jnp.int32, (8, LANES), 0).astype(F32)
    lane = lax.broadcasted_iota(jnp.int32, (8, LANES), 1)
    return sub, lane.astype(F32), lax.rem(lane, TOPK).astype(F32)


def order_pair(rows, columns):
    sub, _, twice = positions()
    pairs = [(wide(row), number_above(columns, wide(row))) for row in rows]
    return as_row(placed(pairs, TOPK // 8, sub), sub, twice)


def best_of_block(total_ref, col_ref):
    sub, lane, _ = positions()
    rows = descending([total_ref[k:k + 1, :] for k in range(8)])
    ranked = ((0, (0,)), (1, (1, 2)), (3, (3, 4, 5, 6, 7)))
    for k, _ in ranked:
        col_ref[k * LANES:(k + 1) * LANES, :] = column_of(rows[k])
    kept = []
    for k, taken in ranked:
        row = wide(rows[k])
        columns = [col_ref[k * LANES + 8 * j:k * LANES + 8 * j + 8, :] for j in range(16)]
        blocks = TOPK // (k + 1) // 8
        if taken == (k,):
            kept += placed([(row, number_above(columns, row))], blocks, sub)
            continue
        before = [
            jnp.where((column > row) | ((column == row) & (sub + float(8 * j) < lane)), 1.0, 0.0)
            for j, column in enumerate(columns)
        ]
        rank = wide(jnp.sum(added(before), axis=0, keepdims=True))
        for block in range(blocks):
            here = rank == sub + float(8 * block)
            for r in taken:
                best = jnp.max(jnp.where(here, wide(rows[r]), -jnp.inf), axis=1, keepdims=True)
                kept.append(jnp.broadcast_to(best, (8, LANES)))
    first = as_row(kept[:16], sub, lane)
    second = jnp.where(lane[:1] < 8.0 * (len(kept) - 16), as_row(kept[16:], sub, lane), -jnp.inf)
    return order_pair([first, second], kept)


def best_of_lists(lists, col_ref):
    lane = lax.broadcasted_iota(jnp.int32, (1, LANES), 1)
    rows = descending(lists)
    low = jnp.full((1, LANES), -jnp.inf, F32)
    packed = []
    for group in ((0, 1, 2, 5), (3, 4) + tuple(range(6, len(rows)))):
        at, line = 0, low
        for s in group:
            if s < len(rows):
                count = TOPK // (s + 1)
                moved = rows[s] if at % TOPK == 0 else pltpu.roll(rows[s], at, 1)
                line = jnp.where((lane >= at) & (lane < at + count), moved, line)
                at += count
        if at:
            packed.append((line, at))
    columns = []
    for k, (line, used) in enumerate(packed):
        col_ref[k * LANES:(k + 1) * LANES, :] = column_of(line)
        columns += [col_ref[k * LANES + 8 * j:k * LANES + 8 * j + 8, :] for j in range(-(-used // 8))]
    return order_pair([line for line, _ in packed], columns)


def merge_last(far, near_columns):
    sub, lane, twice = positions()
    row, first = wide(far), lane < float(TOPK)
    parts, ahead = [], []
    for block, column in enumerate(near_columns):
        count = jnp.sum(jnp.where((row > column) & first, 1.0, 0.0), axis=1, keepdims=True)
        parts.append(jnp.where(count + sub + float(8 * block) == lane, column, 0.0))
        ahead.append(jnp.where(column >= row, 1.0, 0.0))
    place = wide(jnp.sum(added(ahead), axis=0, keepdims=True)) + twice
    for block in range(TOPK // 8):
        slot = sub + float(8 * block)
        value = jnp.sum(jnp.where((place == slot) & first, row, 0.0), axis=1, keepdims=True)
        parts.append(jnp.where(lane == slot, value, 0.0))
    return jnp.sum(added(parts), axis=0, keepdims=True)


def kernel(n_pts, n_cand, points_hbm, weights_hbm, cover_hbm, cand_hbm, picks_hbm, *refs):
    gains_refs, ncov_refs, top_ref = refs[:8], refs[8:16], refs[16]
    (
        points, cands, weights, cover, picks, wcol, ccol, bias, maxes, col,
        part_out, part_in, cov_out, cov_in, top_out, top_in, near_columns, gains,
        p_recv, c_recv, t_recv, near_sem,
    ) = refs[17:]
    farthest = n_cand // 2

    def until_last_list(in_sem, p_send, c_send, t_send, *results):
        n, d = points.shape
        m = cands.shape[0]
        me_p = lax.axis_index("pts")
        me_c = lax.axis_index("cand")

        half = n // 2
        along = sorted(range(1, n_cand), key=lambda k: -min(k, n_cand - k))
        copies = [
            pltpu.make_async_copy(cover_hbm, cover, in_sem.at[0]),
            pltpu.make_async_copy(weights_hbm, weights, in_sem.at[1]),
            pltpu.make_async_copy(picks_hbm, picks, in_sem.at[2]),
            pltpu.make_async_copy(cand_hbm.at[pl.ds(0, m // 2)], cands.at[pl.ds(0, m // 2)], in_sem.at[3]),
            pltpu.make_async_copy(points_hbm.at[pl.ds(0, 256)], points.at[pl.ds(0, 256)], in_sem.at[4]),
            pltpu.make_async_copy(points_hbm.at[pl.ds(256, 256)], points.at[pl.ds(256, 256)], in_sem.at[5]),
            pltpu.make_async_copy(points_hbm.at[pl.ds(half, half)], points.at[pl.ds(half, half)], in_sem.at[6]),
            pltpu.make_async_copy(cand_hbm.at[pl.ds(m // 2, m // 2)], cands.at[pl.ds(m // 2, m // 2)], in_sem.at[7]),
        ]
        for copy in copies:
            copy.start()

        others = [k + lax.div(k - me_p + n_pts - 1, n_pts - 1) for k in range(n_pts - 1)]

        near = 4
        beside = [k for k in range(1, n_cand) if min(k, n_cand - k) <= near]
        barrier = pltpu.get_barrier_semaphore()
        for peer in others:
            pl.semaphore_signal(barrier, 1, device_id={"pts": peer}, device_id_type=pl.DeviceIdType.MESH)
        for k in beside:
            pl.semaphore_signal(barrier, 1, device_id={"cand": lax.rem(me_c + k, n_cand)}, device_id_type=pl.DeviceIdType.MESH)

        copies[0].wait()
        copies[1].wait()
        for k in range(8):
            ccol[k * LANES:(k + 1) * LANES, :] = column_of(cover[k:k + 1, :] * 32.0)
            wcol[k * LANES:(k + 1) * LANES, :] = column_of(weights[k:k + 1, :] * (2.0 ** -20))
        copies[2].wait()
        column = (
            me_c * m
            + lax.broadcasted_iota(jnp.int32, (8, LANES), 0) * LANES
            + lax.broadcasted_iota(jnp.int32, (8, LANES), 1)
        )
        mask = jnp.full((8, LANES), -1e30, F32)
        for k in range(TOPK):
            mask = jnp.where(column == picks[k], 0.0, mask)
        bias[...] = mask
        piece = 128
        held = [[results[(2 * q + u) * 4:(2 * q + u) * 4 + 4] for q in range(2)] for u in range(2)]
        for result in results:
            pltpu.matmul_pop(result)
        sums = [jnp.zeros((8, LANES), F32) for _ in range(8)]
        units = [(0, 256, 0, 4), (256, 256, 0, 5), (half, half, 0, 6), (0, half, 2, None), (half, half, 2, None)]
        steps = [(unit, part) for unit in range(len(units)) for part in range(d // 256)]

        def push(step):
            unit, part = steps[step]
            for q in range(2):
                row = (units[unit][2] + q) * 256
                pltpu.matmul_push_rhs(
                    cands[row:row + 256, part * 256:(part + 1) * 256],
                    staging_register=step % 2, mxu_index=q, transpose=True,
                )

        def accumulate(step):
            unit, part = steps[step]
            first, rows, _, _ = units[unit]
            for p in range(rows // piece):
                for q in range(2):
                    pltpu.matmul_acc_lhs(
                        held[unit % 2][q][p],
                        points[first + p * piece:first + (p + 1) * piece, part * 256:(part + 1) * 256],
                        load_staged_rhs=step % 2 if p == 0 else None,
                    )

        def finish(unit):
            first, rows, tile, _ = units[unit]
            for p in range(rows // piece):
                at = slice(first + p * piece, first + (p + 1) * piece)
                high = None
                for q in range(2):
                    sims = pltpu.matmul_pop(held[unit % 2][q][p])
                    for h in range(2):
                        lane = 2 * (tile + q) + h
                        s = sims[:, h * LANES:(h + 1) * LANES]
                        t = jnp.maximum(s - ccol[at, :], 0.0) * wcol[at, :]
                        sums[lane] = sums[lane] + jnp.sum(t.reshape(piece // 8, 8, LANES), axis=0)
                        masked = s + bias[lane:lane + 1, :]
                        high = masked if high is None else jnp.maximum(high, masked)
                maxes[at, :] = jnp.maximum(maxes[at, :], high) if tile else high

        def send_parts(start, size):
            for k in range(start, start + size):
                part_out[k:k + 1, :] = jnp.sum(sums[k], axis=0, keepdims=True)
            for peer in others:
                pltpu.make_async_remote_copy(
                    part_out.at[pl.ds(start, size)], part_in.at[me_p, pl.ds(start, size)], p_send, p_recv,
                    device_id={"pts": peer}, device_id_type=pl.DeviceIdType.MESH,
                ).start()
            part_in[me_p, start:start + size, :] = part_out[start:start + size, :]

        copies[3].wait()
        push(0)
        for step, (unit, part) in enumerate(steps):
            if step + 1 < len(steps):
                if steps[step + 1] == (3, 0):
                    copies[7].wait()
                push(step + 1)
            if part == 0 and units[unit][3] is not None:
                copies[units[unit][3]].wait()
            accumulate(step)
            if part == 2 and unit > 0:
                finish(unit - 1)
        finish(len(units) - 1)
        pl.semaphore_wait(barrier, n_pts - 1 + len(beside))
        send_parts(0, 8)
        reach, rounds = near, 0
        while reach < n_cand // 2:
            for k in (reach, n_cand - reach):
                pl.semaphore_signal(
                    near_sem.at[rounds], 1, device_id={"cand": lax.rem(me_c + k, n_cand)}, device_id_type=pl.DeviceIdType.MESH
                )
            if rounds == 0:
                for k in range(8):
                    high = maxes[k * LANES:(k + 1) * LANES, :].T
                    cov_out[k:k + 1, :] = jnp.max(high, axis=0, keepdims=True) * (2.0 ** -5)
            pl.semaphore_wait(near_sem.at[rounds], 2)
            reach, rounds = 2 * reach, rounds + 1
        for k in along:
            pltpu.make_async_remote_copy(
                cov_out, cov_in.at[k], c_send, c_recv,
                device_id={"cand": lax.rem(me_c + k, n_cand)}, device_id_type=pl.DeviceIdType.MESH,
            ).start()

        some = part_in.at[pl.ds(0, n_pts - 1)]
        pltpu.make_async_copy(some, some, p_recv).wait()
        total = added([part_in[k] for k in range(n_pts)])
        gains[...] = total
        top_out[...] = best_of_block(gains, col)
        for k in along:
            pltpu.make_async_remote_copy(
                top_out, top_in.at[k], t_send, t_recv.at[int(k == farthest)],
                device_id={"cand": lax.rem(me_c + k, n_cand)}, device_id_type=pl.DeviceIdType.MESH,
            ).start()

        some = cov_in.at[pl.ds(1, n_cand - 1)]
        pltpu.make_async_copy(some, some, c_recv).wait()
        best = jnp.maximum(cover[...], cov_out[...])
        for k in range(1, n_cand):
            best = jnp.maximum(best, cov_in[k])
        for k in range(8):
            gains_refs[k][...] = gains[k:k + 1, :]
            ncov_refs[k][...] = best[k:k + 1, :]

        some = top_in.at[pl.ds(0, n_cand - 2)]
        pltpu.make_async_copy(some, some, t_recv.at[0]).wait()
        near = best_of_lists([top_out[...]] + [top_in[k] for k in range(1, n_cand) if k != farthest], col)
        near_columns[...] = column_of(near)[:TOPK, :]

        for sent, sem, count in ((part_in, p_send, n_pts - 1), (cov_in, c_send, n_cand - 1), (top_in, t_send, n_cand - 1)):
            some = sent.at[pl.ds(0, count)]
            pltpu.make_async_copy(some, some, sem).wait()

    dma = pltpu.SemaphoreType.DMA
    products = [pltpu.ACC(q)((128, 256), F32) for q in range(2) for _ in range(8)]
    pl.run_scoped(until_last_list, dma((8,)), dma, dma, dma, *products)

    some = top_in.at[pl.ds(farthest, 1)]
    pltpu.make_async_copy(some, some, t_recv.at[1]).wait()
    top_ref[...] = merge_last(top_in[farthest], [near_columns[k:k + 8, :] for k in range(0, TOPK, 8)])


def write_out(*refs):
    rows, (gains, ncov, top), (gains_all, ncov_all, best) = refs[:17], refs[17:20], refs[20:]
    best[...] = rows[16][:, :TOPK]
    for k in range(8):
        gains_all[k:k + 1, :] = rows[k][...]
        ncov_all[k:k + 1, :] = rows[8 + k][...]

    def send(sem):
        copies = [
            pltpu.make_async_copy(best, top, sem.at[0]),
            pltpu.make_async_copy(gains_all, gains, sem.at[1]),
            pltpu.make_async_copy(ncov_all, ncov, sem.at[2]),
        ]
        for copy in copies:
            copy.start()
        for copy in copies:
            copy.wait()

    pl.run_scoped(send, pltpu.SemaphoreType.DMA((3,)))


def on_device(points, weights, coverage, candidates, picks):
    n_pts, n_cand = lax.axis_size("pts"), lax.axis_size("cand")
    n, d = points.shape
    m = candidates.shape[0]
    hbm = pl.BlockSpec(memory_space=pl.ANY)
    vmem = pl.BlockSpec(memory_space=pltpu.VMEM)
    dma = pltpu.SemaphoreType.DMA
    inside = pl.pallas_call(
        functools.partial(kernel, n_pts, n_cand),
        out_shape=(jax.ShapeDtypeStruct((1, LANES), F32),) * 17,
        in_specs=[hbm] * 5,
        out_specs=(vmem,) * 17,
        scratch_shapes=[
            pltpu.VMEM((n, d), jnp.bfloat16),
            pltpu.VMEM((m, d), jnp.bfloat16),
            pltpu.VMEM((8, LANES), F32),
            pltpu.VMEM((8, LANES), F32),
            pltpu.SMEM((TOPK,), jnp.int32),
            pltpu.VMEM((n, LANES), F32),
            pltpu.VMEM((n, LANES), F32),
            pltpu.VMEM((8, LANES), F32),
            pltpu.VMEM((n, LANES), F32),
            pltpu.VMEM((1024, LANES), F32),
            pltpu.VMEM((8, LANES), F32),
            pltpu.VMEM((n_pts, 8, LANES), F32),
            pltpu.VMEM((8, LANES), F32),
            pltpu.VMEM((n_cand, 8, LANES), F32),
            pltpu.VMEM((1, LANES), F32),
            pltpu.VMEM((n_cand, 1, LANES), F32),
            pltpu.VMEM((TOPK, LANES), F32),
            pltpu.VMEM((8, LANES), F32),
            dma, dma, dma((2,)), pltpu.SemaphoreType.REGULAR((1,)),
        ],
        compiler_params=pltpu.CompilerParams(
            collective_id=0, has_side_effects=True, vmem_limit_bytes=VMEM_BYTES
        ),
        name="facility",
    )(points, weights.reshape(8, LANES), coverage.reshape(8, LANES), candidates, picks)
    gains, ncov, top = pl.pallas_call(
        write_out,
        out_shape=(
            jax.ShapeDtypeStruct((8, LANES), F32),
            jax.ShapeDtypeStruct((8, LANES), F32),
            jax.ShapeDtypeStruct((1, TOPK), F32),
        ),
        in_specs=[vmem] * 17,
        out_specs=(hbm, hbm, hbm),
        scratch_shapes=[
            pltpu.VMEM((8, LANES), F32), pltpu.VMEM((8, LANES), F32), pltpu.VMEM((1, TOPK), F32)
        ],
        compiler_params=pltpu.CompilerParams(vmem_limit_bytes=2**20),
        name="write_out",
    )(*inside)
    return gains.reshape(m), top.reshape(TOPK), ncov.reshape(n)


def solution(mesh):
    placed = (P("pts", None), P("pts"), P("pts"), P("cand", None), P())
    return jax.shard_map(
        on_device, mesh=mesh, in_specs=placed, out_specs=(P("cand"), P(), P("pts")), check_vma=False
    )
```
